128 devices in a mesh: cls: 4 (over y), dom: 32 (over z, x, core).
Axes of the slice: x: 4, y: 4, z: 4, core: 2. Of those that a mesh axis runs over, the one named last changes fastest.
Arguments:
- particles: bfloat16 [1024, 2, 110592], P(('cls', 'dom')), may hold values from -18 to 18
- labels: int32 [1024, 1], P(('cls', 'dom')), may hold values from 0 to 7; in each aligned block of 8 rows (0 to 7, 8 to 15, ...) at most 2 rows name the same one
- wedge_index: int32 [1024], P(('cls', 'dom')), may hold values from 0 to 11
- wedge_table: float32 [12, 110592], replicated, may hold values from 0.05 to 1
Outputs:
- class_average: float32 [8, 2, 110592], P('cls', None, 'dom')
- weight_total: float32 [8, 110592], P('cls', 'dom')
The draws below stay inside these ranges and needn't reach their ends.
Inputs may be any that keep to these rules, and one draw needn't show every extreme that they name: `labels`: among the rows of one device no class appears more than 2 times, and on some devices one class appears exactly 2 times; every class appears on some device.
All inputs are finite; a program needn't handle non-finite values.
Results may differ from the reference program's by a relative error of at most 0.0003.
Values may be sent and summed in bfloat16 or wider, within the bound.
A program may use at most 128 MiB of HBM per device.

```python
import math
import jax
import jax.numpy as jnp
import numpy as np
from jax import lax

P_DEV = 8
WEDGES = 12
CLASSES = 8
MOST = 2
VOX = 110592
PARTICLES = 1024


def place_ends(values, stream_key, least, top_value):
    dims = values.shape
    index_at = [jax.random.randint(jax.random.fold_in(stream_key, axis), (), 0, dims[axis]) for axis in range(len(dims))]
    values = values.at[tuple(index_at)].set(least)
    longest = dims.index(max(dims))
    index_at[longest] = (index_at[longest] + 1) % dims[longest]
    return values.at[tuple(index_at)].set(top_value)


def level_of(key, shape, pieces, least, high):
    level = 1.0
    for position, parts in pieces:
        draws = jax.random.uniform(jax.random.fold_in(jax.random.fold_in(key, 6), position), (parts,), jnp.float32, least / len(pieces), high / len(pieces))
        level = level * jnp.repeat(jnp.exp(draws), shape[position] // parts).reshape((-1,) + (1,) * (len(shape) - 1 - position))
    return level


def shared_out(own_key, own, number, rows, count, top, limit, slope):
    ranking = jax.random.permutation(own_key, count)
    heavy_load, ordinary = shares(count, rows * top, limit, slope, True), shares(count, rows * top, limit, slope, False)
    places = jnp.arange(count)

    def named(tallies, turn):
        used = int((tallies > 0).sum())
        fixed = max(1, used // 4)
        shifted = fixed + (places - fixed + turn * (used - fixed)) % max(1, count - fixed)
        return jnp.zeros((count,), jnp.int32).at[ranking[jnp.where(places < fixed, places, shifted)]].set(jnp.asarray(tallies, jnp.int32))

    tallies = jnp.where(number % 4 == 0, named(heavy_load, number // 4), named(ordinary, number - number // 4 - 1))
    mixed = jax.random.permutation(jax.random.fold_in(own, 3), count)
    donor, taker = mixed[0:count // 2 * 2:2], mixed[1:count // 2 * 2:2]
    slack = jnp.minimum(tallies[donor] - 1, limit - tallies[taker]) // 2
    slack = jnp.where((donor == ranking[0]) | (taker == ranking[0]) | (tallies[taker] == 0), 0, jnp.maximum(slack, 0))
    shifted = jax.random.randint(jax.random.fold_in(own, 4), (count // 2,), 0, 1 << 20) % (slack + 1)
    tallies = tallies.at[donor].add(-shifted).at[taker].add(shifted)
    items = jnp.searchsorted(jnp.cumsum(tallies), jnp.arange(rows * top), side="right").astype(jnp.int32)
    grid = items.reshape(top, rows).T
    grid = grid[jax.random.permutation(jax.random.fold_in(own, 1), rows)]
    turn = jax.random.randint(jax.random.fold_in(own, 2), (rows, 1), 0, top)
    return jnp.take_along_axis(grid, (jnp.arange(top)[None, :] + turn) % top, axis=1)


def shares(number_of, total, bound, skew, full):
    loads = [(1 << 20) // math.isqrt(standing ** skew) + 1 for standing in range(1, number_of + 1)]
    largest = bound if full else min(bound, max(-(-total // number_of), total * loads[0] // sum(loads)))
    least = 1 if total - largest >= number_of - 1 else 0
    holding, surplus = [largest] + [least] * (number_of - 1), total - largest - least * (number_of - 1)
    while surplus > 0:
        free = [i for i in range(1, number_of) if holding[i] < largest] or [i for i in range(1, number_of) if holding[i] < bound]
        mass, remaining = sum([loads[i] for i in free]), surplus
        for i in free:
            extra = min(bound - holding[i], max(1, remaining * loads[i] // mass), surplus)
            holding[i] = holding[i] + extra
            surplus = surplus - extra
    return np.array(holding)


def bell_draw(rng, shape, spread, limit, split=(), kind=jnp.bfloat16):
    array = spread * jax.random.normal(rng, shape, jnp.float32)
    if split:
        array = array * level_of(rng, shape, split, -0.22, 0.18)
    return jnp.clip(array, -limit, limit).astype(kind)


def setup_inputs(seed: int = 0) -> dict:
    keys = jax.random.split(jax.random.key(seed), 5)
    particles = bell_draw(keys[0], (PARTICLES, 2, VOX), 3.0, 18.0, ((0, 128),))
    labels_keys = jax.random.split(jax.random.fold_in(keys[1], 1), PARTICLES // P_DEV)
    labels_turns = jax.random.permutation(jax.random.fold_in(keys[1], 3), PARTICLES // P_DEV)
    labels = jax.vmap(lambda own, number: shared_out(jax.random.fold_in(keys[1], 2), own, number, P_DEV, CLASSES, 1, MOST, 2))(labels_keys, labels_turns).reshape((PARTICLES, 1))
    wedge_index = place_ends(jax.random.randint(keys[2], (PARTICLES,), 0, WEDGES), jax.random.fold_in(keys[2], 1), 0, WEDGES - 1).astype(jnp.int32)
    wedge_table = jnp.clip(jnp.exp(jax.random.uniform(keys[3], (WEDGES, VOX), jnp.float32, math.log(0.05), math.log(1.0))), 0.05, 1.0)
    return {"particles": particles, "labels": labels, "wedge_index": wedge_index, "wedge_table": wedge_table}


def reference(particles, labels, wedge_index, wedge_table):
    count = particles.shape[0]
    block = 64 if count % 64 == 0 else count
    steps_total = count // block
    classes_all = CLASSES
    label_flat = labels[:, 0]

    def accumulate(carry, index):
        start = (index * block).astype(jnp.int32)
        piece = lax.dynamic_slice_in_dim(particles, start, block, 0).astype(jnp.float32)
        label_piece = lax.dynamic_slice_in_dim(label_flat, start, block, 0)
        wedge_piece = lax.dynamic_slice_in_dim(wedge_index, start, block, 0)
        pick = (wedge_piece[:, None] == jnp.arange(WEDGES, dtype=jnp.int32)[None, :]).astype(jnp.float32)
        weight = jnp.dot(pick, wedge_table, precision=lax.Precision.HIGHEST)
        member = (jnp.arange(classes_all, dtype=jnp.int32)[:, None] == label_piece[None, :]).astype(jnp.float32)
        numer = jnp.einsum("kb,bcv->kcv", member, weight[:, None, :] * piece, precision=lax.Precision.HIGHEST)
        denom = jnp.dot(member, weight * weight, precision=lax.Precision.HIGHEST)
        return (carry[0] + numer, carry[1] + denom), None

    start_sums = (jnp.zeros((classes_all, 2, VOX), jnp.float32), jnp.zeros((classes_all, VOX), jnp.float32))
    (weighted_sum, weight_total), unused = lax.scan(accumulate, start_sums, jnp.arange(steps_total, dtype=jnp.int32))
    class_average = weighted_sum / (weight_total[:, None, :] + 1.0)
    return class_average, weight_total
```

```python
import functools

import jax
import jax.numpy as jnp
from jax import lax
from jax.experimental import pallas as pl
from jax.experimental.pallas import tpu as pltpu
from jax.sharding import PartitionSpec as P

F32 = jnp.float32
BF16 = jnp.bfloat16
MESH = pl.DeviceIdType.MESH
NB = 27
ROWS = 56
WEDGES = 12
PDEV = 8
PIECES = 16
HEAD = 40
TAIL = ROWS - HEAD
STREAM_ROWS = (HEAD, HEAD, 2 * TAIL)
N_COPIES = 21
WINDOW = 64


def kernel(lab, wed, x_hbm, table_hbm, avg_hbm, tot_hbm,
           xo, xp, fo, fp, tb, wexp, lab_p, wed_p, slot_p, slot_w,
           s0, s1, s2, r1_0, r1_1, r1_2, dp_0, dp_1, dp_2, dm_0, dm_1, dm_2,
           r2_0, r2_1, r2_2, ep_0, ep_1, ep_2, em_0, em_1, em_2,
           d3_0, d3_1, d3_2, oa, ow,
           sem_x, sem_t, sem_ps, sem_pr, sem_ls, sem_lr, sem_s, sem_r, sem_o):
    S = (s0, s1, s2)
    R1 = (r1_0, r1_1, r1_2)
    DP = (dp_0, dp_1, dp_2)
    DM = (dm_0, dm_1, dm_2)
    R2 = (r2_0, r2_1, r2_2)
    EP = (ep_0, ep_1, ep_2)
    EM = (em_0, em_1, em_2)
    D3 = (d3_0, d3_1, d3_2)
    y = lax.axis_index("cls")
    dom = lax.axis_index("dom")
    core = lax.rem(dom, 2)
    xc = lax.rem(dom // 2, 4)
    zc = dom // 8

    def device(dz=0, dx=0, dy=0, flip=False):
        c = 1 - core if flip else core
        zz, xx, yy = lax.rem(zc + dz, 4), lax.rem(xc + dx, 4), lax.rem(y + dy, 4)
        return (yy, (zz * 4 + xx) * 2 + c)

    def along(axis, step):
        return device(**{"d" + axis: step})

    partner = device(flip=True)
    AXES = (("x", "z", "y"), ("z", "y", "x"), ("y", "x", "z"))

    barrier = pltpu.get_barrier_semaphore()
    peers = [partner] + [along(a, s) for a in "xyz" for s in (1, 3, 2)]
    for peer in peers:
        pl.semaphore_signal(barrier, inc=1, device_id=peer, device_id_type=MESH)

    def shard_of(piece, c):
        dz, dx = piece // 4, lax.rem(piece, 4)
        return (lax.rem(zc + dz, 4) * 4 + lax.rem(xc + dx, 4)) * 2 + c

    def window(piece, c):
        row = shard_of(piece, c) * (2 * NB)
        start = jnp.minimum(row // 8, (64 * NB - WINDOW) // 8) * 8
        return pl.multiple_of(start, 8), row - start

    def own_copy(piece):
        start, _ = window(piece, core)
        return pltpu.make_async_copy(
            x_hbm.at[:, pl.ds(start, WINDOW)], xo.at[piece], sem_x.at[piece])

    def partner_copy(piece):
        start, _ = window(piece, 1 - core)
        return pltpu.make_async_remote_copy(
            src_ref=x_hbm.at[:, pl.ds(start, WINDOW)], dst_ref=xp.at[piece],
            send_sem=sem_ps.at[piece], recv_sem=sem_pr.at[piece],
            device_id=partner, device_id_type=MESH)

    def start_local(piece, carry):
        start = pl.multiple_of(shard_of(piece, core) * (NB * 128), 128)
        pltpu.make_async_copy(
            table_hbm.at[:, pl.ds(start, NB * 128)], tb.at[piece], sem_t).start()
        own_copy(piece).start()
        return carry

    lax.fori_loop(0, PIECES, start_local, 0)
    pl.semaphore_wait(barrier, len(peers))

    lab_copy = pltpu.make_async_remote_copy(
        src_ref=lab, dst_ref=lab_p, send_sem=sem_ls.at[0], recv_sem=sem_lr.at[0],
        device_id=partner, device_id_type=MESH)
    wed_copy = pltpu.make_async_remote_copy(
        src_ref=wed, dst_ref=wed_p, send_sem=sem_ls.at[1], recv_sem=sem_lr.at[1],
        device_id=partner, device_id_type=MESH)
    lab_copy.start()
    wed_copy.start()

    def start_partner(piece, carry):
        partner_copy(piece).start()
        return carry

    lax.fori_loop(0, PIECES, start_partner, 0)

    def slots(lab_ref, wed_ref, base):
        labels = [lab_ref[p] for p in range(PDEV)]
        wedges = [wed_ref[p] for p in range(PDEV)]

        def one_class(k, carry):
            p1, w1, p2, w2 = 0, WEDGES, 0, WEDGES
            seen = jnp.int32(0)
            for p in range(PDEV):
                hit = labels[p] == k
                first = hit & (seen == 0)
                second = hit & (seen > 0)
                p1 = jnp.where(first, p, p1)
                w1 = jnp.where(first, wedges[p], w1)
                p2 = jnp.where(second, p, p2)
                w2 = jnp.where(second, wedges[p], w2)
                seen = seen + hit.astype(jnp.int32)
            slot_p[k * 4 + base] = p1
            slot_w[k * 4 + base] = w1
            slot_p[k * 4 + base + 1] = p2
            slot_w[k * 4 + base + 1] = w2
            return carry

        lax.fori_loop(0, 8, one_class, 0)

    slots(lab, wed, 0)

    pltpu.make_async_copy(tb, tb, sem_t).wait()

    def expand(piece, carry):
        rows = wexp.at[piece].reshape((WEDGES + 1) * ROWS, 128)
        for b in range(NB):
            for lo, n in ((0, 8), (8, WEDGES - 8)):
                v = tb[piece, pl.ds(lo, n), pl.ds(b * 128, 128)]
                for c in range(2):
                    rows[pl.ds(lo * ROWS + 2 * b + c, n, stride=ROWS), :] = v
        wexp[piece, WEDGES] = jnp.zeros((ROWS, 128), F32)
        return carry

    lax.fori_loop(0, PIECES, expand, 0)

    sub = lax.broadcasted_iota(jnp.int32, (TAIL, 128), 0)
    lane = lax.broadcasted_iota(jnp.int32, (TAIL, 128), 1)

    def term(src, base, k, piece, lo, n):
        total = None
        for s in (base, base + 1):
            p = slot_p[k * 4 + s]
            w = slot_w[k * 4 + s]
            at = window(piece, core)[1]
            v = src[piece, p, pl.ds(at + lo, n), :] * wexp[piece, w, pl.ds(lo, n), :]
            total = v if total is None else total + v
        if lo + n == ROWS:
            count = jnp.zeros((n, 128), F32)
            for s in (base, base + 1):
                count = count + (lane == slot_w[k * 4 + s]).astype(F32)
            total = jnp.where(sub < TAIL - 2, total, jnp.where(sub == TAIL - 2, count, 0.0))
        return total

    def group(step):
        return lax.rem(y + step, 4) * 2

    def sums(stream, ra, rb, src, base, add):
        for rc in range(4):
            if stream == 0:
                parts = [(0, term(src, base, group(rc), rb * 4 + ra, 0, HEAD))]
            elif stream == 1:
                parts = [(0, term(src, base, group(rb) + 1, ra * 4 + rc, 0, HEAD))]
            else:
                parts = [(j * TAIL, term(src, base, group(ra) + j, rc * 4 + rb, HEAD, TAIL))
                         for j in range(2)]
            for at, v in parts:
                rows = pl.ds(at, v.shape[0])
                if add:
                    v = v + S[stream][ra, rb, rc, rows, :]
                S[stream][ra, rb, rc, rows, :] = v

    def unpack(src, dst, piece):
        def body(p, carry):
            dst[piece, p, pl.ds(0, WINDOW), :] = src[piece, p].astype(F32)
            return carry
        lax.fori_loop(0, PDEV, body, 0, unroll=True)

    def wait_own(piece, carry):
        own_copy(piece).wait()
        unpack(xo, fo, piece)
        return carry

    lax.fori_loop(0, PIECES, wait_own, 0)

    def own_pass(ra, carry):
        def inner(rb, c):
            for stream in range(3):
                sums(stream, ra, rb, fo, 0, False)
            return c
        return lax.fori_loop(0, 4, inner, carry)

    lax.fori_loop(0, 4, own_pass, 0)

    lab_copy.wait()
    wed_copy.wait()
    slots(lab_p, wed_p, 2)

    def wait_partner(piece, carry):
        partner_copy(piece).wait()
        unpack(xp, fp, piece)
        return carry

    lax.fori_loop(0, PIECES, wait_partner, 0)

    def copy(stream, i, src, dst, level, step):
        return pltpu.make_async_remote_copy(
            src_ref=src, dst_ref=dst, send_sem=sem_s.at[stream, i], recv_sem=sem_r.at[stream, i],
            device_id=along(AXES[stream][level], step), device_id_type=MESH)

    def relay1(t, rb):
        return copy(t, rb, S[t].at[2, rb], R1[t].at[rb], 0, 1 if rb >= 2 else 3)

    def own1(t, rb):
        if rb >= 2:
            return copy(t, 4 + rb, S[t].at[3, rb], DM[t].at[rb], 0, 3)
        return copy(t, 4 + rb, S[t].at[1, rb], DP[t].at[rb], 0, 1)

    def comb1(t, rb):
        if rb >= 2:
            return copy(t, 8 + rb, S[t].at[1, rb], DP[t].at[rb], 0, 1)
        return copy(t, 8 + rb, S[t].at[3, rb], DM[t].at[rb], 0, 3)

    HALF = (pl.ds(0, 2), pl.ds(2, 2))

    def relay2(t, h):
        return copy(t, 12 + h, S[t].at[0, 2, HALF[h]], R2[t].at[HALF[h]], 1, 1 if h else 3)

    def own2(t, h):
        if h:
            return copy(t, 14 + h, S[t].at[0, 3, HALF[h]], EM[t].at[HALF[h]], 1, 3)
        return copy(t, 14 + h, S[t].at[0, 1, HALF[h]], EP[t].at[HALF[h]], 1, 1)

    def comb2(t, h):
        if h:
            return copy(t, 16 + h, S[t].at[0, 1, HALF[h]], EP[t].at[HALF[h]], 1, 1)
        return copy(t, 16 + h, S[t].at[0, 3, HALF[h]], EM[t].at[HALF[h]], 1, 3)

    def last3(t, rc):
        return copy(t, 17 + rc, S[t].at[0, 0, rc], D3[t].at[rc - 1], 2, rc)

    started = []

    def go(c):
        c.start()
        started.append(c)

    for rb in (2, 1, 3, 0):
        for t in range(3):
            sums(t, 2, rb, fp, 2, True)
            go(relay1(t, rb))
    for rb in (1, 2, 0, 3):
        for t in range(3):
            sums(t, 1 if rb < 2 else 3, rb, fp, 2, True)
            go(own1(t, rb))
    for rb in (2, 1, 3, 0):
        for t in range(3):
            sums(t, 1 if rb >= 2 else 3, rb, fp, 2, True)

    def zero_pass(rb, carry):
        for t in range(3):
            sums(t, 0, rb, fp, 2, True)
        return carry

    lax.fori_loop(0, 4, zero_pass, 0)

    for rb in (2, 1, 3, 0):
        for t in range(3):
            relay1(t, rb).wait_recv()
            ra = 1 if rb >= 2 else 3
            S[t][ra, rb] = S[t][ra, rb] + R1[t][rb]
            go(comb1(t, rb))
    for rb in (2, 1, 3, 0):
        for t in range(3):
            own1(t, rb).wait_recv()
            comb1(t, rb).wait_recv()
            S[t][0, rb] = S[t][0, rb] + DP[t][rb] + DM[t][rb]
            if rb == 2:
                go(relay2(t, 0))
                go(relay2(t, 1))
            elif rb == 1:
                go(own2(t, 0))
                relay2(t, 1).wait_recv()
                S[t][0, 1, 2:4] = S[t][0, 1, 2:4] + R2[t][2:4]
                go(comb2(t, 1))
            elif rb == 3:
                go(own2(t, 1))
                relay2(t, 0).wait_recv()
                S[t][0, 3, 0:2] = S[t][0, 3, 0:2] + R2[t][0:2]
                go(comb2(t, 0))
    for t in range(3):
        for h in (1, 0):
            own2(t, h).wait_recv()
            comb2(t, h).wait_recv()
        S[t][0, 0] = S[t][0, 0] + EP[t][...] + EM[t][...]
        for rc in (2, 1, 3):
            go(last3(t, rc))
    final = []
    for t in (2, 0, 1):
        for rc in (1, 3, 2):
            last3(t, rc).wait_recv()
        final.append(S[t][0, 0, 0] + D3[t][0] + D3[t][1] + D3[t][2])
    tail, heads = final[0], final[1:]

    counts_lane = lax.broadcasted_iota(jnp.int32, (1, 128), 1)
    even = lax.rem(lax.broadcasted_iota(jnp.int32, (ROWS, 128), 0), 2) == 0
    totals = []
    for j in range(2):
        row = tail[j * TAIL + TAIL - 2:j * TAIL + TAIL - 1, :]
        total = jnp.zeros((ROWS, 128), F32)
        for w in range(WEDGES):
            n = jnp.sum(jnp.where(counts_lane == w, row, 0.0), axis=1, keepdims=True)
            a = wexp[0, w]
            total = total + n * (a * a)
        totals.append(total)
        summed = jnp.concatenate([heads[j], tail[j * TAIL:(j + 1) * TAIL]], axis=0)
        avg = summed / (total + 1.0)
        oa[j] = avg[0:2 * NB].reshape(NB, 2, 128)
    ow[...] = jnp.where(even, totals[0], totals[1])[0:2 * NB].reshape(NB, 2, 128)
    o1 = pltpu.make_async_copy(oa, avg_hbm, sem_o.at[0])
    o2 = pltpu.make_async_copy(ow, tot_hbm, sem_o.at[1])
    o1.start()
    o2.start()
    for c in started:
        c.wait_send()
    o1.wait()
    o2.wait()


def per_device(particles, labels, wedge_index, wedge_table):
    x = particles.reshape(PDEV, 2, 32 * NB, 128).transpose(0, 2, 1, 3)
    x = x.reshape(PDEV, 64 * NB, 128)
    lab = labels.reshape(PDEV)
    smem = pl.BlockSpec(memory_space=pltpu.SMEM)
    hbm = pl.BlockSpec(memory_space=pl.ANY)
    dma = pltpu.SemaphoreType.DMA
    V = pltpu.VMEM

    def per_stream(*lead):
        return [V((*lead, r, 128), F32) for r in STREAM_ROWS]

    avg, tot = pl.pallas_call(
        kernel,
        out_shape=(jax.ShapeDtypeStruct((2, NB, 2, 128), F32),
                   jax.ShapeDtypeStruct((NB, 2, 128), F32)),
        in_specs=[smem, smem, hbm, hbm],
        out_specs=(hbm, hbm),
        scratch_shapes=[
            V((PIECES, PDEV, WINDOW, 128), BF16),
            V((PIECES, PDEV, WINDOW, 128), BF16),
            V((PIECES, PDEV, WINDOW + 8, 128), F32),
            V((PIECES, PDEV, WINDOW + 8, 128), F32),
            V((PIECES, WEDGES, NB * 128), F32),
            V((PIECES, WEDGES + 1, ROWS, 128), F32),
            pltpu.SMEM((PDEV,), jnp.int32),
            pltpu.SMEM((PDEV,), jnp.int32),
            pltpu.SMEM((32,), jnp.int32),
            pltpu.SMEM((32,), jnp.int32),
            *per_stream(4, 4, 4),
            *per_stream(4, 4), *per_stream(4, 4), *per_stream(4, 4),
            *per_stream(4), *per_stream(4), *per_stream(4),
            *per_stream(3),
            V((2, NB, 2, 128), F32),
            V((NB, 2, 128), F32),
            dma((PIECES,)), dma(()), dma((PIECES,)), dma((PIECES,)), dma((2,)), dma((2,)),
            dma((3, N_COPIES)), dma((3, N_COPIES)), dma((2,)),
        ],
        compiler_params=pltpu.CompilerParams(
            collective_id=0, has_side_effects=True, vmem_limit_bytes=60 * 1024 * 1024),
        name="class_sums",
    )(lab, wedge_index, x, wedge_table)
    avg = avg.transpose(0, 2, 1, 3).reshape(2, 2, NB * 128)
    tot = tot.transpose(1, 0, 2).reshape(2, NB * 128)
    return avg, tot


def solution(mesh):
    return jax.shard_map(
        per_device,
        mesh=mesh,
        in_specs=(P(("cls", "dom"), None, None), P(("cls", "dom"), None), P(("cls", "dom")), P()),
        out_specs=(P("cls", None, "dom"), P("cls", "dom")),
        check_vma=False,
    )
```

```python
import jax
import jax.numpy as jnp
from jax import lax
from jax.experimental import pallas as pl
from jax.experimental.pallas import tpu as pltpu
from jax.sharding import PartitionSpec as P

F32 = jnp.float32
BF16 = jnp.bfloat16
MESH = pl.DeviceIdType.MESH
NB = 27
ROWS = 56
WEDGES = 12
PDEV = 8
PIECES = 16
HEAD = 40
TAIL = ROWS - HEAD
STREAM_ROWS = (HEAD, HEAD, 2 * TAIL)
N_COPIES = 21
WINDOW = 64
AXES = (("x", "z", "y"), ("z", "y", "x"), ("y", "x", "z"))
ORDER = ((2, 2), (3, 2), (1, 2), (0, 2), (2, 3), (2, 1), (2, 0), (3, 3),
         (1, 3), (0, 3), (1, 1), (0, 1), (3, 1), (1, 0), (3, 0), (0, 0))


def kernel(lab_hbm, wed_hbm, x_hbm, table_hbm, avg_ref, tot_ref,
           xo, xp, fo, fp, tb, wexp, lab, wed, lab_p, wed_p, slot_p, slot_w,
           s0, s1, s2, r1_0, r1_1, r1_2, dp_0, dp_1, dp_2, dm_0, dm_1, dm_2,
           r2_0, r2_1, r2_2, ep_0, ep_1, ep_2, em_0, em_1, em_2,
           d3_0, d3_1, d3_2,
           sem_x, sem_t, sem_l, sem_ps, sem_pr, sem_ls, sem_lr, sem_s, sem_r):
    S = (s0, s1, s2)
    R1 = (r1_0, r1_1, r1_2)
    DP = (dp_0, dp_1, dp_2)
    DM = (dm_0, dm_1, dm_2)
    R2 = (r2_0, r2_1, r2_2)
    EP = (ep_0, ep_1, ep_2)
    EM = (em_0, em_1, em_2)
    D3 = (d3_0, d3_1, d3_2)
    y = lax.axis_index("cls")
    dom = lax.axis_index("dom")
    core = lax.rem(dom, 2)
    xc = lax.rem(dom // 2, 4)
    zc = dom // 8

    def device(dz=0, dx=0, dy=0, flip=False):
        c = 1 - core if flip else core
        zz, xx, yy = lax.rem(zc + dz, 4), lax.rem(xc + dx, 4), lax.rem(y + dy, 4)
        return (yy, (zz * 4 + xx) * 2 + c)

    def along(axis, step):
        return device(**{"d" + axis: step})

    partner = device(flip=True)
    barrier = pltpu.get_barrier_semaphore()
    peers = [partner] + [along(a, s) for a in "xyz" for s in (1, 3, 2)]
    for peer in peers:
        pl.semaphore_signal(barrier, inc=1, device_id=peer, device_id_type=MESH)

    def shard_of(piece, c):
        dz, dx = piece // 4, piece % 4
        return (lax.rem(zc + dz, 4) * 4 + lax.rem(xc + dx, 4)) * 2 + c

    def window(piece, c):
        row = shard_of(piece, c) * (2 * NB)
        start = jnp.minimum(row // 8, (64 * NB - WINDOW) // 8) * 8
        return pl.multiple_of(start, 8), row - start

    def own_copy(piece):
        start, _ = window(piece, core)
        return pltpu.make_async_copy(
            x_hbm.at[:, pl.ds(start, WINDOW)], xo.at[piece], sem_x.at[piece])

    def table_copy(piece):
        start = pl.multiple_of(shard_of(piece, core) * (NB * 128), 128)
        return pltpu.make_async_copy(
            table_hbm.at[:, pl.ds(start, NB * 128)], tb.at[piece], sem_t.at[piece])

    def partner_copy(piece):
        start, _ = window(piece, 1 - core)
        return pltpu.make_async_remote_copy(
            src_ref=x_hbm.at[:, pl.ds(start, WINDOW)], dst_ref=xp.at[piece],
            send_sem=sem_ps.at[piece], recv_sem=sem_pr.at[piece],
            device_id=partner, device_id_type=MESH)

    order = [dz * 4 + dx for dz, dx in ORDER]
    lab_local = pltpu.make_async_copy(lab_hbm, lab, sem_l.at[0])
    wed_local = pltpu.make_async_copy(wed_hbm, wed, sem_l.at[1])
    lab_local.start()
    wed_local.start()
    for piece in order:
        table_copy(piece).start()
        own_copy(piece).start()
    pl.semaphore_wait(barrier, len(peers))

    lab_copy = pltpu.make_async_remote_copy(
        src_ref=lab_hbm, dst_ref=lab_p, send_sem=sem_ls.at[0], recv_sem=sem_lr.at[0],
        device_id=partner, device_id_type=MESH)
    wed_copy = pltpu.make_async_remote_copy(
        src_ref=wed_hbm, dst_ref=wed_p, send_sem=sem_ls.at[1], recv_sem=sem_lr.at[1],
        device_id=partner, device_id_type=MESH)
    lab_copy.start()
    wed_copy.start()
    for piece in order:
        partner_copy(piece).start()

    def slots(lab_ref, wed_ref, base):
        labels = [lab_ref[p] for p in range(PDEV)]
        wedges = [wed_ref[p] for p in range(PDEV)]

        def one_class(k, carry):
            p1, w1, p2, w2 = 0, WEDGES, 0, WEDGES
            seen = jnp.int32(0)
            for p in range(PDEV):
                hit = labels[p] == k
                first = hit & (seen == 0)
                second = hit & (seen > 0)
                p1 = jnp.where(first, p, p1)
                w1 = jnp.where(first, wedges[p], w1)
                p2 = jnp.where(second, p, p2)
                w2 = jnp.where(second, wedges[p], w2)
                seen = seen + hit.astype(jnp.int32)
            slot_p[k * 4 + base] = p1
            slot_w[k * 4 + base] = w1
            slot_p[k * 4 + base + 1] = p2
            slot_w[k * 4 + base + 1] = w2
            return carry

        lax.fori_loop(0, 8, one_class, 0)

    lab_local.wait()
    wed_local.wait()
    slots(lab, wed, 0)

    def expand(piece):
        rows = wexp.at[piece].reshape((WEDGES + 1) * ROWS, 128)
        for b in range(NB):
            for lo, n in ((0, 8), (8, WEDGES - 8)):
                v = tb[piece, pl.ds(lo, n), pl.ds(b * 128, 128)]
                for c in range(2):
                    rows[pl.ds(lo * ROWS + 2 * b + c, n, stride=ROWS), :] = v
        wexp[piece, WEDGES] = jnp.zeros((ROWS, 128), F32)

    def unpack(src, dst, piece):
        def body(p, carry):
            dst[piece, p, pl.ds(0, WINDOW), :] = src[piece, p].astype(F32)
            return carry
        lax.fori_loop(0, PDEV, body, 0, unroll=True)

    for piece in order:
        table_copy(piece).wait()
        own_copy(piece).wait()
        expand(piece)
        unpack(xo, fo, piece)

    lab_copy.wait()
    wed_copy.wait()
    slots(lab_p, wed_p, 2)

    sub = lax.broadcasted_iota(jnp.int32, (TAIL, 128), 0)
    lane = lax.broadcasted_iota(jnp.int32, (TAIL, 128), 1)

    def class_sum(dz, dx, at, dy, j):
        piece = dz * 4 + dx
        k = lax.rem(y + dy, 4) * 2 + j
        total = None
        count = jnp.zeros((TAIL, 128), F32)
        for s in range(4):
            p = slot_p[k * 4 + s]
            w = slot_w[k * 4 + s]
            src = fo if s < 2 else fp
            v = src[piece, p, pl.ds(at, ROWS), :] * wexp[piece, w]
            total = v if total is None else total + v
            count = count + (lane == w).astype(F32)
        tail = jnp.where(sub < TAIL - 2, total[HEAD:ROWS],
                         jnp.where(sub == TAIL - 2, count, 0.0))
        if j == 0:
            S[0][dx, dz, pl.ds(dy * HEAD, HEAD), :] = total[0:HEAD]
        else:
            S[1][dz, dy, pl.ds(dx * HEAD, HEAD), :] = total[0:HEAD]
        S[2][dy, dx, pl.ds(dz * 2 * TAIL + j * TAIL, TAIL), :] = tail

    def copy(stream, i, src, dst, level, step):
        return pltpu.make_async_remote_copy(
            src_ref=src, dst_ref=dst, send_sem=sem_s.at[stream, i], recv_sem=sem_r.at[stream, i],
            device_id=along(AXES[stream][level], step), device_id_type=MESH)

    def relay1(t, rb):
        return copy(t, rb, S[t].at[2, rb], R1[t].at[rb], 0, 1 if rb >= 2 else 3)

    def own1(t, rb):
        if rb >= 2:
            return copy(t, 4 + rb, S[t].at[3, rb], DM[t].at[rb], 0, 3)
        return copy(t, 4 + rb, S[t].at[1, rb], DP[t].at[rb], 0, 1)

    def comb1(t, rb):
        if rb >= 2:
            return copy(t, 8 + rb, S[t].at[1, rb], DP[t].at[rb], 0, 1)
        return copy(t, 8 + rb, S[t].at[3, rb], DM[t].at[rb], 0, 3)

    def half(t, h):
        n = 2 * STREAM_ROWS[t]
        return pl.ds(h * n, n)

    def relay2(t, h):
        return copy(t, 12 + h, S[t].at[0, 2, half(t, h)], R2[t].at[half(t, h)], 1, 1 if h else 3)

    def own2(t, h):
        if h:
            return copy(t, 14 + h, S[t].at[0, 3, half(t, h)], EM[t].at[half(t, h)], 1, 3)
        return copy(t, 14 + h, S[t].at[0, 1, half(t, h)], EP[t].at[half(t, h)], 1, 1)

    def comb2(t, h):
        if h:
            return copy(t, 16 + h, S[t].at[0, 1, half(t, h)], EP[t].at[half(t, h)], 1, 1)
        return copy(t, 16 + h, S[t].at[0, 3, half(t, h)], EM[t].at[half(t, h)], 1, 3)

    def last3(t, rc):
        n = STREAM_ROWS[t]
        return copy(t, 17 + rc, S[t].at[0, 0, pl.ds(rc * n, n)], D3[t].at[rc - 1], 2, rc)

    started = []

    def go(c):
        c.start()
        started.append(c)

    done = set()
    sent = set()
    sends = ([(0, relay1, rb, [(rb, 2)]) for rb in (2, 1, 3, 0)]
             + [(2, relay1, 2, [(d, 2) for d in range(4)])]
             + [(1, relay1, rb, [(2, d) for d in range(4)]) for rb in (2, 1, 3, 0)]
             + [(2, relay1, rb, [(d, rb) for d in range(4)]) for rb in (1, 3, 0)]
             + [(0, own1, rb, [(rb, 1 if rb < 2 else 3)]) for rb in (1, 2, 0, 3)]
             + [(1, own1, rb, [(1 if rb < 2 else 3, d) for d in range(4)]) for rb in (1, 2, 0, 3)]
             + [(2, own1, rb, [(d, rb) for d in range(4)]) for rb in (1, 2, 0, 3)])
    for dz, dx in ORDER:
        piece = dz * 4 + dx
        partner_copy(piece).wait()
        unpack(xp, fp, piece)
        at = window(piece, core)[1]

        def classes(dy, carry):
            for j in range(2):
                class_sum(dz, dx, at, dy, j)
            return carry

        lax.fori_loop(0, 4, classes, 0)
        done.add((dz, dx))
        for i, (t, make, rb, needs) in enumerate(sends):
            if i not in sent and done.issuperset(needs):
                sent.add(i)
                go(make(t, rb))

    for rb in (2, 1, 3, 0):
        for t in range(3):
            relay1(t, rb).wait_recv()
            ra = 1 if rb >= 2 else 3
            S[t][ra, rb] = S[t][ra, rb] + R1[t][rb]
            go(comb1(t, rb))
    for rb in (2, 1, 3, 0):
        for t in range(3):
            own1(t, rb).wait_recv()
            comb1(t, rb).wait_recv()
            S[t][0, rb] = S[t][0, rb] + DP[t][rb] + DM[t][rb]
            if rb == 2:
                go(relay2(t, 0))
                go(relay2(t, 1))
            elif rb == 1:
                go(own2(t, 0))
            elif rb == 3:
                go(own2(t, 1))
    for t in range(3):
        for h in (1, 0):
            relay2(t, h).wait_recv()
            rb = 1 if h else 3
            S[t][0, rb, half(t, h)] = S[t][0, rb, half(t, h)] + R2[t][half(t, h)]
            go(comb2(t, h))
    for t in range(3):
        for h in (1, 0):
            own2(t, h).wait_recv()
            comb2(t, h).wait_recv()
        S[t][0, 0] = S[t][0, 0] + EP[t][...] + EM[t][...]
        for rc in (2, 1, 3):
            go(last3(t, rc))
    final = []
    for t in (2, 0, 1):
        for rc in (1, 3, 2):
            last3(t, rc).wait_recv()
        final.append(S[t][0, 0, pl.ds(0, STREAM_ROWS[t])] + D3[t][0] + D3[t][1] + D3[t][2])
    tail, heads = final[0], final[1:]

    counts_lane = lax.broadcasted_iota(jnp.int32, (1, 128), 1)
    even = lax.rem(lax.broadcasted_iota(jnp.int32, (ROWS, 128), 0), 2) == 0
    totals = []
    for j in range(2):
        row = tail[j * TAIL + TAIL - 2:j * TAIL + TAIL - 1, :]
        total = jnp.zeros((ROWS, 128), F32)
        for w in range(WEDGES):
            n = jnp.sum(jnp.where(counts_lane == w, row, 0.0), axis=1, keepdims=True)
            a = wexp[0, w]
            total = total + n * (a * a)
        totals.append(total)
        summed = jnp.concatenate([heads[j], tail[j * TAIL:(j + 1) * TAIL]], axis=0)
        avg = summed / (total + 1.0)
        avg_ref[j] = avg[0:2 * NB].reshape(NB, 2, 128)
    tot_ref[...] = jnp.where(even, totals[0], totals[1])[0:2 * NB].reshape(NB, 2, 128)
    for c in started:
        c.wait_send()


def put_out(avg_ref, tot_ref, avg_out, tot_out, sems):
    one = pltpu.make_async_copy(avg_ref, avg_out, sems.at[0])
    two = pltpu.make_async_copy(tot_ref, tot_out, sems.at[1])
    one.start()
    two.start()
    one.wait()
    two.wait()


def per_device(particles, labels, wedge_index, wedge_table):
    x = particles.reshape(PDEV, 2, 32 * NB, 128).transpose(0, 2, 1, 3)
    x = x.reshape(PDEV, 64 * NB, 128)
    lab = labels.reshape(PDEV)
    hbm = pl.BlockSpec(memory_space=pltpu.HBM)
    vmem = pl.BlockSpec(memory_space=pltpu.VMEM)
    dma = pltpu.SemaphoreType.DMA
    V = pltpu.VMEM

    def per_stream(*lead, n=1):
        return [V((*lead, n * r, 128), F32) for r in STREAM_ROWS]

    shapes = (jax.ShapeDtypeStruct((2, NB, 2, 128), F32),
              jax.ShapeDtypeStruct((NB, 2, 128), F32))
    avg, tot = pl.pallas_call(
        kernel,
        out_shape=shapes,
        in_specs=[hbm] * 4,
        out_specs=(vmem, vmem),
        scratch_shapes=[
            V((PIECES, PDEV, WINDOW, 128), BF16),
            V((PIECES, PDEV, WINDOW, 128), BF16),
            V((PIECES, PDEV, WINDOW + 8, 128), F32),
            V((PIECES, PDEV, WINDOW + 8, 128), F32),
            V((PIECES, WEDGES, NB * 128), F32),
            V((PIECES, WEDGES + 1, ROWS, 128), F32),
            *[pltpu.SMEM((PDEV,), jnp.int32)] * 4,
            pltpu.SMEM((32,), jnp.int32),
            pltpu.SMEM((32,), jnp.int32),
            *per_stream(4, 4, n=4),
            *per_stream(4, n=4), *per_stream(4, n=4), *per_stream(4, n=4),
            *per_stream(n=4), *per_stream(n=4), *per_stream(n=4),
            *per_stream(3),
            dma((PIECES,)), dma((PIECES,)), dma((2,)), dma((PIECES,)), dma((PIECES,)),
            dma((2,)), dma((2,)), dma((3, N_COPIES)), dma((3, N_COPIES)),
        ],
        compiler_params=pltpu.CompilerParams(
            collective_id=0, has_side_effects=True, vmem_limit_bytes=44 * 1024 * 1024),
        name="class_sums",
    )(*[pltpu.with_memory_space_constraint(a, pltpu.HBM) for a in (lab, wedge_index, x, wedge_table)])
    avg, tot = pl.pallas_call(
        put_out,
        out_shape=shapes,
        in_specs=[vmem] * 2,
        out_specs=(hbm, hbm),
        scratch_shapes=[dma((2,))],
        compiler_params=pltpu.CompilerParams(vmem_limit_bytes=1024 * 1024),
        name="put_out",
    )(avg, tot)
    avg = avg.transpose(0, 2, 1, 3).reshape(2, 2, NB * 128)
    tot = tot.transpose(1, 0, 2).reshape(2, NB * 128)
    return avg, tot


def solution(mesh):
    return jax.shard_map(
        per_device,
        mesh=mesh,
        in_specs=(P(("cls", "dom"), None, None), P(("cls", "dom"), None), P(("cls", "dom")), P()),
        out_specs=(P("cls", None, "dom"), P("cls", "dom")),
        check_vma=False,
    )
```

```python
import jax
import jax.numpy as jnp
from jax import lax
from jax.experimental import pallas as pl
from jax.experimental.pallas import tpu as pltpu
from jax.sharding import PartitionSpec as P

F32 = jnp.float32
BF16 = jnp.bfloat16
MESH = pl.DeviceIdType.MESH
NB = 27
ROWS = 56
WEDGES = 12
PDEV = 8
PIECES = 16
HEAD = 40
TAIL = ROWS - HEAD
STREAM_ROWS = (HEAD, HEAD, 2 * TAIL)
N_COPIES = 21
WINDOW = 64
TOP = 32700.0
STEPS = 64.0
LN2 = 0.6931471805599453
AXES = (("x", "z", "y"), ("z", "y", "x"), ("y", "x", "z"))
ORDER = ((2, 2), (3, 2), (1, 2), (0, 2), (2, 3), (2, 1), (2, 0), (3, 3),
         (1, 3), (0, 3), (1, 1), (0, 1), (3, 1), (1, 0), (3, 0), (0, 0))


def kernel(lab_hbm, wed_hbm, x_hbm, table_hbm, avg_ref, tot_ref,
           xo, xp, fo, fp, tb, wexp, lab, wed, lab_p, wed_p, slot_p, slot_w,
           s0, s1, s2, qs_0, qs_1, qs_2, q1_0, q1_1, q1_2, qp_0, qp_1, qp_2, qm_0, qm_1, qm_2,
           r2_0, r2_1, r2_2, ep_0, ep_1, ep_2, em_0, em_1, em_2,
           d3_0, d3_1, d3_2,
           sem_x, sem_t, sem_l, sem_ps, sem_pr, sem_ls, sem_lr, sem_s, sem_r):
    S = (s0, s1, s2)
    QS = (qs_0, qs_1, qs_2)
    Q1 = (q1_0, q1_1, q1_2)
    QP = (qp_0, qp_1, qp_2)
    QM = (qm_0, qm_1, qm_2)
    R2 = (r2_0, r2_1, r2_2)
    EP = (ep_0, ep_1, ep_2)
    EM = (em_0, em_1, em_2)
    D3 = (d3_0, d3_1, d3_2)
    y = lax.axis_index("cls")
    dom = lax.axis_index("dom")
    core = lax.rem(dom, 2)
    xc = lax.rem(dom // 2, 4)
    zc = dom // 8

    def device(dz=0, dx=0, dy=0, flip=False):
        c = 1 - core if flip else core
        zz, xx, yy = lax.rem(zc + dz, 4), lax.rem(xc + dx, 4), lax.rem(y + dy, 4)
        return (yy, (zz * 4 + xx) * 2 + c)

    def along(axis, step):
        return device(**{"d" + axis: step})

    partner = device(flip=True)
    barrier = pltpu.get_barrier_semaphore()
    peers = [partner] + [along(a, s) for a in "xyz" for s in (1, 3, 2)]
    for peer in peers:
        pl.semaphore_signal(barrier, inc=1, device_id=peer, device_id_type=MESH)

    def shard_of(piece, c):
        dz, dx = piece // 4, piece % 4
        return (lax.rem(zc + dz, 4) * 4 + lax.rem(xc + dx, 4)) * 2 + c

    def window(piece, c):
        row = shard_of(piece, c) * (2 * NB)
        start = jnp.minimum(row // 8, (64 * NB - WINDOW) // 8) * 8
        return pl.multiple_of(start, 8), row - start

    def own_copy(piece):
        start, _ = window(piece, core)
        return pltpu.make_async_copy(
            x_hbm.at[:, pl.ds(start, WINDOW)], xo.at[piece], sem_x.at[piece])

    def table_copy(piece):
        start = pl.multiple_of(shard_of(piece, core) * (NB * 128), 128)
        return pltpu.make_async_copy(
            table_hbm.at[:, pl.ds(start, NB * 128)], tb.at[piece], sem_t.at[piece])

    def partner_copy(piece):
        start, _ = window(piece, 1 - core)
        return pltpu.make_async_remote_copy(
            src_ref=x_hbm.at[:, pl.ds(start, WINDOW)], dst_ref=xp.at[piece],
            send_sem=sem_ps.at[piece], recv_sem=sem_pr.at[piece],
            device_id=partner, device_id_type=MESH)

    order = [dz * 4 + dx for dz, dx in ORDER]
    lab_local = pltpu.make_async_copy(lab_hbm, lab, sem_l.at[0])
    wed_local = pltpu.make_async_copy(wed_hbm, wed, sem_l.at[1])
    lab_local.start()
    wed_local.start()
    for piece in order:
        table_copy(piece).start()
        own_copy(piece).start()
    pl.semaphore_wait(barrier, len(peers))

    lab_copy = pltpu.make_async_remote_copy(
        src_ref=lab_hbm, dst_ref=lab_p, send_sem=sem_ls.at[0], recv_sem=sem_lr.at[0],
        device_id=partner, device_id_type=MESH)
    wed_copy = pltpu.make_async_remote_copy(
        src_ref=wed_hbm, dst_ref=wed_p, send_sem=sem_ls.at[1], recv_sem=sem_lr.at[1],
        device_id=partner, device_id_type=MESH)
    lab_copy.start()
    wed_copy.start()
    for piece in order:
        partner_copy(piece).start()

    def slots(lab_ref, wed_ref, base):
        labels = [lab_ref[p] for p in range(PDEV)]
        wedges = [wed_ref[p] for p in range(PDEV)]

        def one_class(k, carry):
            p1, w1, p2, w2 = 0, WEDGES, 0, WEDGES
            seen = jnp.int32(0)
            for p in range(PDEV):
                hit = labels[p] == k
                first = hit & (seen == 0)
                second = hit & (seen > 0)
                p1 = jnp.where(first, p, p1)
                w1 = jnp.where(first, wedges[p], w1)
                p2 = jnp.where(second, p, p2)
                w2 = jnp.where(second, wedges[p], w2)
                seen = seen + hit.astype(jnp.int32)
            slot_p[k * 4 + base] = p1
            slot_w[k * 4 + base] = w1
            slot_p[k * 4 + base + 1] = p2
            slot_w[k * 4 + base + 1] = w2
            return carry

        lax.fori_loop(0, 8, one_class, 0)

    lab_local.wait()
    wed_local.wait()
    slots(lab, wed, 0)

    def expand(piece):
        rows = wexp.at[piece].reshape((WEDGES + 1) * ROWS, 128)
        for b in range(NB):
            for lo, n in ((0, 8), (8, WEDGES - 8)):
                v = tb[piece, pl.ds(lo, n), pl.ds(b * 128, 128)]
                for c in range(2):
                    rows[pl.ds(lo * ROWS + 2 * b + c, n, stride=ROWS), :] = v
        wexp[piece, WEDGES] = jnp.zeros((ROWS, 128), F32)

    def unpack(src, dst, piece):
        def body(p, carry):
            dst[piece, p, pl.ds(0, WINDOW), :] = src[piece, p].astype(F32)
            return carry
        lax.fori_loop(0, PDEV, body, 0, unroll=True)

    for piece in order:
        table_copy(piece).wait()
        own_copy(piece).wait()
        expand(piece)
        unpack(xo, fo, piece)

    lab_copy.wait()
    wed_copy.wait()
    slots(lab_p, wed_p, 2)

    sub = lax.broadcasted_iota(jnp.int32, (TAIL, 128), 0)
    sub8 = lax.broadcasted_iota(jnp.int32, (8, 128), 0)
    lane8 = lax.broadcasted_iota(jnp.int32, (8, 128), 1)

    def chip_counts(dy):
        total = jnp.zeros((8, 128), F32)
        for j in range(2):
            k = lax.rem(y + dy, 4) * 2 + j
            for s in range(4):
                total = total + ((lane8 == slot_w[k * 4 + s]) & (sub8 == j)).astype(F32)
        return total

    def encode(t, dst, v, counts):
        n = 4 * STREAM_ROWS[t]
        v = v.reshape(n // 8, 8, 128)
        top = jnp.maximum(jnp.max(jnp.abs(v), axis=0), 1e-30)
        code = jnp.ceil(jnp.log(top) * (STEPS / LN2))
        q = jnp.round(v * (jnp.exp(code * (-LN2 / STEPS)) * TOP)[None])
        dst[pl.ds(0, n), :] = q.reshape(n, 128).astype(jnp.int32).astype(jnp.int16)
        extra = jnp.concatenate([code, counts], axis=0)
        dst[pl.ds(n, 16), :] = extra.astype(jnp.int32).astype(jnp.int16)

    def decode(t, src):
        n = 4 * STREAM_ROWS[t]
        q = src[pl.ds(0, n), :].astype(jnp.int32).astype(F32)
        extra = src[pl.ds(n, 16), :].astype(jnp.int32).astype(F32)
        scale = jnp.exp(extra[0:8] * (LN2 / STEPS)) * (1.0 / TOP)
        return (q.reshape(n // 8, 8, 128) * scale[None]).reshape(n, 128), extra[8:16]

    def class_sum(dz, dx, at, dy, j):
        piece = dz * 4 + dx
        k = lax.rem(y + dy, 4) * 2 + j
        total = None
        for s in range(4):
            p = slot_p[k * 4 + s]
            w = slot_w[k * 4 + s]
            src = fo if s < 2 else fp
            v = src[piece, p, pl.ds(at, ROWS), :] * wexp[piece, w]
            total = v if total is None else total + v
        tail = jnp.where(sub < TAIL - 2, total[HEAD:ROWS], 0.0)
        if j == 0:
            S[0][dx, dz, pl.ds(dy * HEAD, HEAD), :] = total[0:HEAD]
        else:
            S[1][dz, dy, pl.ds(dx * HEAD, HEAD), :] = total[0:HEAD]
        S[2][dy, dx, pl.ds(dz * 2 * TAIL + j * TAIL, TAIL), :] = tail

    def copy(stream, i, src, dst, level, step):
        return pltpu.make_async_remote_copy(
            src_ref=src, dst_ref=dst, send_sem=sem_s.at[stream, i], recv_sem=sem_r.at[stream, i],
            device_id=along(AXES[stream][level], step), device_id_type=MESH)

    def relay1(t, rb):
        return copy(t, rb, QS[t].at[rb], Q1[t].at[rb], 0, 1 if rb >= 2 else 3)

    def own1(t, rb):
        if rb >= 2:
            return copy(t, 4 + rb, QS[t].at[4 + rb], QM[t].at[rb], 0, 3)
        return copy(t, 4 + rb, QS[t].at[4 + rb], QP[t].at[rb], 0, 1)

    def comb1(t, rb):
        if rb >= 2:
            return copy(t, 8 + rb, QS[t].at[8 + rb], QP[t].at[rb], 0, 1)
        return copy(t, 8 + rb, QS[t].at[8 + rb], QM[t].at[rb], 0, 3)

    none = jnp.zeros((8, 128), F32)

    def counts_of(t, ra):
        return chip_counts(ra) if t == 2 else none

    def half(t, h):
        n = 2 * STREAM_ROWS[t]
        return pl.ds(h * n, n)

    def relay2(t, h):
        return copy(t, 12 + h, S[t].at[0, 2, half(t, h)], R2[t].at[half(t, h)], 1, 1 if h else 3)

    def own2(t, h):
        if h:
            return copy(t, 14 + h, S[t].at[0, 3, half(t, h)], EM[t].at[half(t, h)], 1, 3)
        return copy(t, 14 + h, S[t].at[0, 1, half(t, h)], EP[t].at[half(t, h)], 1, 1)

    def comb2(t, h):
        if h:
            return copy(t, 16 + h, S[t].at[0, 1, half(t, h)], EP[t].at[half(t, h)], 1, 1)
        return copy(t, 16 + h, S[t].at[0, 3, half(t, h)], EM[t].at[half(t, h)], 1, 3)

    def last3(t, rc):
        n = STREAM_ROWS[t]
        return copy(t, 17 + rc, S[t].at[0, 0, pl.ds(rc * n, n)], D3[t].at[rc - 1], 2, rc)

    row = lax.broadcasted_iota(jnp.int32, (8 * TAIL, 128), 0)
    count_rows = [lax.rem(row, 2 * TAIL) == j * TAIL + TAIL - 2 for j in range(2)]
    started = []

    def go(c):
        c.start()
        started.append(c)

    done = set()
    sent = set()
    sends = ([(0, relay1, rb, [(rb, 2)]) for rb in (2, 1, 3, 0)]
             + [(2, relay1, 2, [(d, 2) for d in range(4)])]
             + [(1, relay1, rb, [(2, d) for d in range(4)]) for rb in (2, 1, 3, 0)]
             + [(2, relay1, rb, [(d, rb) for d in range(4)]) for rb in (1, 3, 0)]
             + [(0, own1, rb, [(rb, 1 if rb < 2 else 3)]) for rb in (1, 2, 0, 3)]
             + [(1, own1, rb, [(1 if rb < 2 else 3, d) for d in range(4)]) for rb in (1, 2, 0, 3)]
             + [(2, own1, rb, [(d, rb) for d in range(4)]) for rb in (1, 2, 0, 3)])
    for dz, dx in ORDER:
        piece = dz * 4 + dx
        partner_copy(piece).wait()
        unpack(xp, fp, piece)
        at = window(piece, core)[1]

        def classes(dy, carry):
            for j in range(2):
                class_sum(dz, dx, at, dy, j)
            return carry

        lax.fori_loop(0, 4, classes, 0)
        done.add((dz, dx))
        for i, (t, make, rb, needs) in enumerate(sends):
            if i not in sent and done.issuperset(needs):
                sent.add(i)
                ra = 2 if make is relay1 else (3 if rb >= 2 else 1)
                place = rb if make is relay1 else 4 + rb
                encode(t, QS[t].at[place], S[t][ra, rb], counts_of(t, ra))
                go(make(t, rb))

    for rb in (2, 1, 3, 0):
        for t in range(3):
            relay1(t, rb).wait_recv()
            ra = 1 if rb >= 2 else 3
            v, c = decode(t, Q1[t].at[rb])
            encode(t, QS[t].at[8 + rb], S[t][ra, rb] + v, counts_of(t, ra) + c)
            go(comb1(t, rb))
    for rb in (2, 1, 3, 0):
        for t in range(3):
            own1(t, rb).wait_recv()
            comb1(t, rb).wait_recv()
            vp, cp = decode(t, QP[t].at[rb])
            vm, cm = decode(t, QM[t].at[rb])
            total = S[t][0, rb] + vp + vm
            if t == 2:
                if rb == 2:
                    ring_counts = chip_counts(0) + cp + cm
                for j in range(2):
                    total = total + jnp.where(count_rows[j], ring_counts[j:j + 1], 0.0)
            S[t][0, rb] = total
            if rb == 2:
                go(relay2(t, 0))
                go(relay2(t, 1))
            elif rb == 1:
                go(own2(t, 0))
            elif rb == 3:
                go(own2(t, 1))
    for t in range(3):
        for h in (1, 0):
            relay2(t, h).wait_recv()
            rb = 1 if h else 3
            S[t][0, rb, half(t, h)] = S[t][0, rb, half(t, h)] + R2[t][half(t, h)]
            go(comb2(t, h))
    for t in range(3):
        for h in (1, 0):
            own2(t, h).wait_recv()
            comb2(t, h).wait_recv()
        S[t][0, 0] = S[t][0, 0] + EP[t][...] + EM[t][...]
        for rc in (2, 1, 3):
            go(last3(t, rc))
    final = []
    for t in (2, 0, 1):
        for rc in (1, 3, 2):
            last3(t, rc).wait_recv()
        final.append(S[t][0, 0, pl.ds(0, STREAM_ROWS[t])] + D3[t][0] + D3[t][1] + D3[t][2])
    tail, heads = final[0], final[1:]

    counts_lane = lax.broadcasted_iota(jnp.int32, (1, 128), 1)
    even = lax.rem(lax.broadcasted_iota(jnp.int32, (ROWS, 128), 0), 2) == 0
    totals = []
    for j in range(2):
        row = tail[j * TAIL + TAIL - 2:j * TAIL + TAIL - 1, :]
        total = jnp.zeros((ROWS, 128), F32)
        for w in range(WEDGES):
            n = jnp.sum(jnp.where(counts_lane == w, row, 0.0), axis=1, keepdims=True)
            a = wexp[0, w]
            total = total + n * (a * a)
        totals.append(total)
        summed = jnp.concatenate([heads[j], tail[j * TAIL:(j + 1) * TAIL]], axis=0)
        avg = summed / (total + 1.0)
        avg_ref[j] = avg[0:2 * NB].reshape(NB, 2, 128)
    tot_ref[...] = jnp.where(even, totals[0], totals[1])[0:2 * NB].reshape(NB, 2, 128)
    for c in started:
        c.wait_send()


def put_out(avg_ref, tot_ref, avg_out, tot_out, sems):
    one = pltpu.make_async_copy(avg_ref, avg_out, sems.at[0])
    two = pltpu.make_async_copy(tot_ref, tot_out, sems.at[1])
    one.start()
    two.start()
    one.wait()
    two.wait()


def per_device(particles, labels, wedge_index, wedge_table):
    x = particles.reshape(PDEV, 2, 32 * NB, 128).transpose(0, 2, 1, 3)
    x = x.reshape(PDEV, 64 * NB, 128)
    lab = labels.reshape(PDEV)
    hbm = pl.BlockSpec(memory_space=pltpu.HBM)
    vmem = pl.BlockSpec(memory_space=pltpu.VMEM)
    dma = pltpu.SemaphoreType.DMA
    V = pltpu.VMEM

    def per_stream(*lead, n=1):
        return [V((*lead, n * r, 128), F32) for r in STREAM_ROWS]

    def coded(n):
        return [V((n, 4 * r + 16, 128), jnp.int16) for r in STREAM_ROWS]

    shapes = (jax.ShapeDtypeStruct((2, NB, 2, 128), F32),
              jax.ShapeDtypeStruct((NB, 2, 128), F32))
    avg, tot = pl.pallas_call(
        kernel,
        out_shape=shapes,
        in_specs=[hbm] * 4,
        out_specs=(vmem, vmem),
        scratch_shapes=[
            V((PIECES, PDEV, WINDOW, 128), BF16),
            V((PIECES, PDEV, WINDOW, 128), BF16),
            V((PIECES, PDEV, WINDOW + 8, 128), F32),
            V((PIECES, PDEV, WINDOW + 8, 128), F32),
            V((PIECES, WEDGES, NB * 128), F32),
            V((PIECES, WEDGES + 1, ROWS, 128), F32),
            *[pltpu.SMEM((PDEV,), jnp.int32)] * 4,
            pltpu.SMEM((32,), jnp.int32),
            pltpu.SMEM((32,), jnp.int32),
            *per_stream(4, 4, n=4),
            *coded(12), *coded(4), *coded(4), *coded(4),
            *per_stream(n=4), *per_stream(n=4), *per_stream(n=4),
            *per_stream(3),
            dma((PIECES,)), dma((PIECES,)), dma((2,)), dma((PIECES,)), dma((PIECES,)),
            dma((2,)), dma((2,)), dma((3, N_COPIES)), dma((3, N_COPIES)),
        ],
        compiler_params=pltpu.CompilerParams(
            collective_id=0, has_side_effects=True, vmem_limit_bytes=44 * 1024 * 1024),
        name="class_sums",
    )(*[pltpu.with_memory_space_constraint(a, pltpu.HBM) for a in (lab, wedge_index, x, wedge_table)])
    avg, tot = pl.pallas_call(
        put_out,
        out_shape=shapes,
        in_specs=[vmem] * 2,
        out_specs=(hbm, hbm),
        scratch_shapes=[dma((2,))],
        compiler_params=pltpu.CompilerParams(vmem_limit_bytes=1024 * 1024),
        name="put_out",
    )(avg, tot)
    avg = avg.transpose(0, 2, 1, 3).reshape(2, 2, NB * 128)
    tot = tot.transpose(1, 0, 2).reshape(2, NB * 128)
    return avg, tot


def solution(mesh):
    return jax.shard_map(
        per_device,
        mesh=mesh,
        in_specs=(P(("cls", "dom"), None, None), P(("cls", "dom"), None), P(("cls", "dom")), P()),
        out_specs=(P("cls", None, "dom"), P("cls", "dom")),
        check_vma=False,
    )
```

```python
import jax
import jax.numpy as jnp
from jax import lax
from jax.experimental import pallas as pl
from jax.experimental.pallas import tpu as pltpu
from jax.sharding import PartitionSpec as P

F32 = jnp.float32
BF16 = jnp.bfloat16
MESH = pl.DeviceIdType.MESH
NB = 27
ROWS = 56
WEDGES = 12
PDEV = 8
PIECES = 16
HEAD = 40
TAIL = ROWS - HEAD
STREAM_ROWS = (HEAD, HEAD, 2 * TAIL)
WINDOW = 64
TOP = 32700.0
STEPS = 64.0
LN2 = 0.6931471805599453
AXES = (("x", "z", "y"), ("z", "y", "x"), ("y", "x", "z"))
ORDER = ((2, 2), (3, 2), (1, 2), (0, 2), (2, 3), (2, 1), (2, 0), (3, 3),
         (1, 3), (0, 3), (1, 1), (0, 1), (3, 1), (1, 0), (3, 0), (0, 0))


def kernel(lab_hbm, wed_hbm, x_hbm, table_hbm, avg_ref, tot_ref,
           xo, xp, fo, fp, tb, wexp, lab, wed, lab_p, wed_p, slot_p, slot_w,
           s0, s1, s2, qs_0, qs_1, qs_2, q1_0, q1_1, q1_2, qd_0, qd_1, qd_2,
           qt_0, qt_1, qt_2, qf_0, qf_1, qf_2,
           sem_x, sem_t, sem_l, sem_ps, sem_pr, sem_ls, sem_lr,
           sem_s1, sem_s2, sem_r1, sem_rd, sem_rf):
    S = (s0, s1, s2)
    QS = (qs_0, qs_1, qs_2)
    Q1 = (q1_0, q1_1, q1_2)
    QD = (qd_0, qd_1, qd_2)
    QT = (qt_0, qt_1, qt_2)
    QF = (qf_0, qf_1, qf_2)
    y = lax.axis_index("cls")
    dom = lax.axis_index("dom")
    core = lax.rem(dom, 2)
    xc = lax.rem(dom // 2, 4)
    zc = dom // 8

    def device(dz=0, dx=0, dy=0, flip=False):
        c = 1 - core if flip else core
        zz, xx, yy = lax.rem(zc + dz, 4), lax.rem(xc + dx, 4), lax.rem(y + dy, 4)
        return (yy, (zz * 4 + xx) * 2 + c)

    def along(axis, step):
        return device(**{"d" + axis: step})

    partner = device(flip=True)
    barrier = pltpu.get_barrier_semaphore()
    peers = [partner] + [along(a, s) for a in "xyz" for s in (1, 3, 2)]
    for peer in peers:
        pl.semaphore_signal(barrier, inc=1, device_id=peer, device_id_type=MESH)

    def shard_of(pos, c):
        dz, dx = ORDER[pos]
        return (lax.rem(zc + dz, 4) * 4 + lax.rem(xc + dx, 4)) * 2 + c

    def window(pos, c):
        row = shard_of(pos, c) * (2 * NB)
        start = jnp.minimum(row // 8, (64 * NB - WINDOW) // 8) * 8
        return pl.multiple_of(start, 8), row - start

    def own_copy(pos):
        start, _ = window(pos, core)
        return pltpu.make_async_copy(
            x_hbm.at[:, pl.ds(start, WINDOW)], xo.at[pos], sem_x.at[pos // 4])

    def table_copy(pos):
        start = pl.multiple_of(shard_of(pos, core) * (NB * 128), 128)
        return pltpu.make_async_copy(
            table_hbm.at[:, pl.ds(start, NB * 128)], tb.at[pos], sem_t.at[pos // 4])

    def batch_of(pos):
        return (pos + 2) // 3

    def partner_copy(pos):
        start, _ = window(pos, 1 - core)
        return pltpu.make_async_remote_copy(
            src_ref=x_hbm.at[:, pl.ds(start, WINDOW)], dst_ref=xp.at[pos],
            send_sem=sem_ps, recv_sem=sem_pr.at[batch_of(pos)],
            device_id=partner, device_id_type=MESH)

    def wait_bytes(ref, sem):
        pltpu.make_async_copy(ref, ref, sem).wait()

    lab_local = pltpu.make_async_copy(lab_hbm, lab, sem_l.at[0])
    wed_local = pltpu.make_async_copy(wed_hbm, wed, sem_l.at[1])
    lab_local.start()
    wed_local.start()
    for pos in range(PIECES):
        table_copy(pos).start()
        own_copy(pos).start()
    pl.semaphore_wait(barrier, len(peers))

    lab_copy = pltpu.make_async_remote_copy(
        src_ref=lab_hbm, dst_ref=lab_p, send_sem=sem_ls.at[0], recv_sem=sem_lr.at[0],
        device_id=partner, device_id_type=MESH)
    wed_copy = pltpu.make_async_remote_copy(
        src_ref=wed_hbm, dst_ref=wed_p, send_sem=sem_ls.at[1], recv_sem=sem_lr.at[1],
        device_id=partner, device_id_type=MESH)
    lab_copy.start()
    wed_copy.start()
    for pos in range(PIECES):
        partner_copy(pos).start()

    def slots(lab_ref, wed_ref, base):
        labels = [lab_ref[p] for p in range(PDEV)]
        wedges = [wed_ref[p] for p in range(PDEV)]

        def one_class(k, carry):
            p1, w1, p2, w2 = 0, WEDGES, 0, WEDGES
            seen = jnp.int32(0)
            for p in range(PDEV):
                hit = labels[p] == k
                first = hit & (seen == 0)
                second = hit & (seen > 0)
                p1 = jnp.where(first, p, p1)
                w1 = jnp.where(first, wedges[p], w1)
                p2 = jnp.where(second, p, p2)
                w2 = jnp.where(second, wedges[p], w2)
                seen = seen + hit.astype(jnp.int32)
            slot_p[k * 4 + base] = p1
            slot_w[k * 4 + base] = w1
            slot_p[k * 4 + base + 1] = p2
            slot_w[k * 4 + base + 1] = w2
            return carry

        lax.fori_loop(0, 8, one_class, 0)

    lab_local.wait()
    wed_local.wait()
    slots(lab, wed, 0)

    def expand(piece):
        rows = wexp.at[piece].reshape((WEDGES + 1) * ROWS, 128)
        for b in range(NB):
            for lo, n in ((0, 8), (8, WEDGES - 8)):
                v = tb[piece, pl.ds(lo, n), pl.ds(b * 128, 128)]
                for c in range(2):
                    rows[pl.ds(lo * ROWS + 2 * b + c, n, stride=ROWS), :] = v
        wexp[piece, WEDGES] = jnp.zeros((ROWS, 128), F32)

    def unpack(src, dst, piece):
        def body(p, carry):
            dst[piece, p, pl.ds(0, WINDOW), :] = src[piece, p].astype(F32)
            return carry
        lax.fori_loop(0, PDEV, body, 0, unroll=True)

    for pos in range(PIECES):
        if pos % 4 == 0:
            wait_bytes(tb.at[pl.ds(pos, 4)], sem_t.at[pos // 4])
            wait_bytes(xo.at[pl.ds(pos, 4)], sem_x.at[pos // 4])
        expand(pos)
        unpack(xo, fo, pos)

    lab_copy.wait_recv()
    wed_copy.wait_recv()
    slots(lab_p, wed_p, 2)

    sub = lax.broadcasted_iota(jnp.int32, (TAIL, 128), 0)
    sub8 = lax.broadcasted_iota(jnp.int32, (8, 128), 0)
    lane8 = lax.broadcasted_iota(jnp.int32, (8, 128), 1)

    def chip_counts(dy):
        total = jnp.zeros((8, 128), F32)
        for j in range(2):
            k = lax.rem(y + dy, 4) * 2 + j
            for s in range(4):
                total = total + ((lane8 == slot_w[k * 4 + s]) & (sub8 == j)).astype(F32)
        return total

    def encode(dst, v, *more):
        n = v.shape[0]
        v = v.reshape(n // 8, 8, 128)
        top = jnp.maximum(jnp.max(jnp.abs(v), axis=0), 1e-30)
        code = jnp.ceil(jnp.log(top) * (STEPS / LN2))
        q = jnp.round(v * (jnp.exp(code * (-LN2 / STEPS)) * TOP)[None])
        rows = jnp.concatenate([q.reshape(n, 128), code, *more], axis=0)
        dst[...] = rows.astype(jnp.int32).astype(jnp.int16)

    def decode(src, n):
        rows = src[...].astype(jnp.int32).astype(F32)
        scale = jnp.exp(rows[n:n + 8] * (LN2 / STEPS)) * (1.0 / TOP)
        return (rows[0:n].reshape(n // 8, 8, 128) * scale[None]).reshape(n, 128), rows[n + 8:]

    def class_sum(piece, at, dy, j):
        dz, dx = ORDER[piece]
        k = lax.rem(y + dy, 4) * 2 + j
        total = None
        for s in range(4):
            p = slot_p[k * 4 + s]
            w = slot_w[k * 4 + s]
            src = fo if s < 2 else fp
            v = src[piece, p, pl.ds(at, ROWS), :] * wexp[piece, w]
            total = v if total is None else total + v
        tail = jnp.where(sub < TAIL - 2, total[HEAD:ROWS], 0.0)
        if j == 0:
            S[0][dx, dz, pl.ds(dy * HEAD, HEAD), :] = total[0:HEAD]
        else:
            S[1][dz, dy, pl.ds(dx * HEAD, HEAD), :] = total[0:HEAD]
        S[2][dy, dx, pl.ds(dz * 2 * TAIL + j * TAIL, TAIL), :] = tail

    def ring(t, src, dst, recv, step):
        return pltpu.make_async_remote_copy(
            src_ref=src, dst_ref=dst, send_sem=sem_s1.at[t], recv_sem=recv,
            device_id=along(AXES[t][0], step), device_id_type=MESH)

    def relay1(t, rb):
        return ring(t, QS[t].at[rb], Q1[t].at[rb], sem_r1.at[t, rb], 1 if rb >= 2 else 3)

    def own1(t, rb):
        side = 1 if rb >= 2 else 0
        return ring(t, QS[t].at[4 + rb], QD[t].at[rb, side], sem_rd.at[t, rb], 3 if side else 1)

    def comb1(t, rb):
        side = 0 if rb >= 2 else 1
        return ring(t, QS[t].at[8 + rb], QD[t].at[rb, side], sem_rd.at[t, rb], 3 if side else 1)

    def plane(t, rb, rc):
        m = rb * 4 + rc - 1
        target = device(**{"d" + AXES[t][1]: rb, "d" + AXES[t][2]: rc})
        return pltpu.make_async_remote_copy(
            src_ref=QT[t].at[m], dst_ref=QF[t].at[m],
            send_sem=sem_s2.at[t], recv_sem=sem_rf.at[t],
            device_id=target, device_id_type=MESH)

    none = jnp.zeros((8, 128), F32)

    def counts_of(t, ra):
        return chip_counts(ra) if t == 2 else none

    def half(t, h):
        n = 2 * STREAM_ROWS[t]
        return pl.ds(h * n, n)

    def relay2(t, h):
        return copy(t, 12 + h, S[t].at[0, 2, half(t, h)], R2[t].at[half(t, h)], 1, 1 if h else 3)

    def own2(t, h):
        if h:
            return copy(t, 14 + h, S[t].at[0, 3, half(t, h)], EM[t].at[half(t, h)], 1, 3)
        return copy(t, 14 + h, S[t].at[0, 1, half(t, h)], EP[t].at[half(t, h)], 1, 1)

    def comb2(t, h):
        if h:
            return copy(t, 16 + h, S[t].at[0, 1, half(t, h)], EP[t].at[half(t, h)], 1, 1)
        return copy(t, 16 + h, S[t].at[0, 3, half(t, h)], EM[t].at[half(t, h)], 1, 3)

    def last3(t, rc):
        n = STREAM_ROWS[t]
        return copy(t, 17 + rc, S[t].at[0, 0, pl.ds(rc * n, n)], D3[t].at[rc - 1], 2, rc)

    done = set()
    sent = set()
    sends = ([(0, relay1, rb, [(rb, 2)]) for rb in (2, 1, 3, 0)]
             + [(2, relay1, 2, [(d, 2) for d in range(4)])]
             + [(1, relay1, rb, [(2, d) for d in range(4)]) for rb in (2, 1, 3, 0)]
             + [(2, relay1, rb, [(d, rb) for d in range(4)]) for rb in (1, 3, 0)]
             + [(0, own1, rb, [(rb, 1 if rb < 2 else 3)]) for rb in (1, 2, 0, 3)]
             + [(1, own1, rb, [(1 if rb < 2 else 3, d) for d in range(4)]) for rb in (1, 2, 0, 3)]
             + [(2, own1, rb, [(d, rb) for d in range(4)]) for rb in (1, 2, 0, 3)])
    for pos in range(PIECES):
        if pos == 0 or batch_of(pos) != batch_of(pos - 1):
            batch = [p for p in range(PIECES) if batch_of(p) == batch_of(pos)]
            wait_bytes(xp.at[pl.ds(pos, len(batch))], sem_pr.at[batch_of(pos)])
        unpack(xp, fp, pos)
        at = window(pos, core)[1]

        def classes(dy, carry):
            for j in range(2):
                class_sum(pos, at, dy, j)
            return carry

        lax.fori_loop(0, 4, classes, 0)
        done.add(ORDER[pos])
        for i, (t, make, rb, needs) in enumerate(sends):
            if i not in sent and done.issuperset(needs):
                sent.add(i)
                ra = 2 if make is relay1 else (3 if rb >= 2 else 1)
                place = rb if make is relay1 else 4 + rb
                encode(QS[t].at[place], S[t][ra, rb], counts_of(t, ra))
                make(t, rb).start()

    for rb in (2, 1, 3, 0):
        for t in range(3):
            n = 4 * STREAM_ROWS[t]
            relay1(t, rb).wait_recv()
            ra = 1 if rb >= 2 else 3
            v, c = decode(Q1[t].at[rb], n)
            encode(QS[t].at[8 + rb], S[t][ra, rb] + v, counts_of(t, ra) + c)
            comb1(t, rb).start()
    kept = [None] * 3
    for rb in (2, 1, 3, 0):
        for t in range(3):
            wait_bytes(QD[t].at[rb], sem_rd.at[t, rb])
        for t in range(3):
            r = STREAM_ROWS[t]
            v0, c0 = decode(QD[t].at[rb, 0], 4 * r)
            v1, c1 = decode(QD[t].at[rb, 1], 4 * r)
            total = S[t][0, rb] + v0 + v1
            more = ()
            if t == 2:
                if rb == 2:
                    counts = chip_counts(0) + c0 + c1
                more = (counts,)
            for rc in (2, 1, 3, 0):
                part = total[rc * r:(rc + 1) * r]
                if rb or rc:
                    encode(QT[t].at[rb * 4 + rc - 1], part, *more)
                    plane(t, rb, rc).start()
                else:
                    kept[t] = part
    final = []
    for t in (2, 0, 1):
        wait_bytes(QF[t], sem_rf.at[t])
        total = kept[t]
        for m in range(15):
            v, c = decode(QF[t].at[m], STREAM_ROWS[t])
            total = total + v
            if t == 2:
                counts = counts + c
        final.append(total)
    tail, heads = final[0], final[1:]

    counts_lane = lax.broadcasted_iota(jnp.int32, (1, 128), 1)
    even = lax.rem(lax.broadcasted_iota(jnp.int32, (ROWS, 128), 0), 2) == 0
    totals = []
    for j in range(2):
        row = counts[j:j + 1]
        total = jnp.zeros((ROWS, 128), F32)
        for w in range(WEDGES):
            n = jnp.sum(jnp.where(counts_lane == w, row, 0.0), axis=1, keepdims=True)
            a = wexp[PIECES - 1, w]
            total = total + n * (a * a)
        totals.append(total)
        summed = jnp.concatenate([heads[j], tail[j * TAIL:(j + 1) * TAIL]], axis=0)
        avg = summed / (total + 1.0)
        avg_ref[j] = avg[0:2 * NB].reshape(NB, 2, 128)
    tot_ref[...] = jnp.where(even, totals[0], totals[1])[0:2 * NB].reshape(NB, 2, 128)
    for t in range(3):
        wait_bytes(QS[t], sem_s1.at[t])
        wait_bytes(QT[t], sem_s2.at[t])
    wait_bytes(xp, sem_ps)
    lab_copy.wait_send()
    wed_copy.wait_send()


def put_out(avg_ref, tot_ref, avg_out, tot_out, sems):
    one = pltpu.make_async_copy(avg_ref, avg_out, sems.at[0])
    two = pltpu.make_async_copy(tot_ref, tot_out, sems.at[1])
    one.start()
    two.start()
    one.wait()
    two.wait()


def per_device(particles, labels, wedge_index, wedge_table):
    x = particles.reshape(PDEV, 2, 32 * NB, 128).transpose(0, 2, 1, 3)
    x = x.reshape(PDEV, 64 * NB, 128)
    lab = labels.reshape(PDEV)
    hbm = pl.BlockSpec(memory_space=pltpu.HBM)
    vmem = pl.BlockSpec(memory_space=pltpu.VMEM)
    dma = pltpu.SemaphoreType.DMA
    V = pltpu.VMEM

    def per_stream(*lead):
        return [V((*lead, 4 * r, 128), F32) for r in STREAM_ROWS]

    def coded(*lead):
        return [V((*lead, 4 * r + 16, 128), jnp.int16) for r in STREAM_ROWS]

    shapes = (jax.ShapeDtypeStruct((2, NB, 2, 128), F32),
              jax.ShapeDtypeStruct((NB, 2, 128), F32))
    avg, tot = pl.pallas_call(
        kernel,
        out_shape=shapes,
        in_specs=[hbm] * 4,
        out_specs=(vmem, vmem),
        scratch_shapes=[
            V((PIECES, PDEV, WINDOW, 128), BF16),
            V((PIECES, PDEV, WINDOW, 128), BF16),
            V((PIECES, PDEV, WINDOW + 8, 128), F32),
            V((PIECES, PDEV, WINDOW + 8, 128), F32),
            V((PIECES, WEDGES, NB * 128), F32),
            V((PIECES, WEDGES + 1, ROWS, 128), F32),
            *[pltpu.SMEM((PDEV,), jnp.int32)] * 4,
            pltpu.SMEM((32,), jnp.int32),
            pltpu.SMEM((32,), jnp.int32),
            *per_stream(4, 4),
            *coded(12), *coded(4), *coded(4, 2),
            *[V((15, HEAD + 8, 128), jnp.int16)] * 6,
            dma((4,)), dma((4,)), dma((2,)), dma(()), dma((6,)), dma((2,)), dma((2,)),
            dma((3,)), dma((3,)), dma((3, 4)), dma((3, 4)), dma((3,)),
        ],
        compiler_params=pltpu.CompilerParams(
            collective_id=0, has_side_effects=True, vmem_limit_bytes=44 * 1024 * 1024),
        name="class_sums",
    )(*[pltpu.with_memory_space_constraint(a, pltpu.HBM) for a in (lab, wedge_index, x, wedge_table)])
    avg, tot = pl.pallas_call(
        put_out,
        out_shape=shapes,
        in_specs=[vmem] * 2,
        out_specs=(hbm, hbm),
        scratch_shapes=[dma((2,))],
        compiler_params=pltpu.CompilerParams(vmem_limit_bytes=1024 * 1024),
        name="put_out",
    )(avg, tot)
    avg = avg.transpose(0, 2, 1, 3).reshape(2, 2, NB * 128)
    tot = tot.transpose(1, 0, 2).reshape(2, NB * 128)
    return avg, tot


def solution(mesh):
    return jax.shard_map(
        per_device,
        mesh=mesh,
        in_specs=(P(("cls", "dom"), None, None), P(("cls", "dom"), None), P(("cls", "dom")), P()),
        out_specs=(P("cls", None, "dom"), P("cls", "dom")),
        check_vma=False,
    )
```

```python
import jax
import jax.numpy as jnp
from jax import lax
from jax.experimental import pallas as pl
from jax.experimental.pallas import tpu as pltpu
from jax.sharding import PartitionSpec as P

F32 = jnp.float32
BF16 = jnp.bfloat16
MESH = pl.DeviceIdType.MESH
NB = 27
ROWS = 56
WEDGES = 12
PDEV = 8
PIECES = 16
HEAD = 40
TAIL = ROWS - HEAD
STREAM_ROWS = (HEAD, HEAD, 2 * TAIL)
WINDOW = 64
TOP = 32700.0
STEPS = 64.0
LN2 = 0.6931471805599453
AXES = (("x", "z", "y"), ("z", "x", "y"), ("y", "x", "z"))
ORDER = ((2, 2), (1, 2), (2, 1), (3, 2), (2, 3), (0, 2), (2, 0), (1, 1),
         (0, 1), (3, 1), (3, 3), (1, 3), (0, 3), (1, 0), (3, 0), (0, 0))
BATCH = (0, 1, 2, 3, 4, 5, 5, 6, 6, 6, 7, 7, 7, 8, 8, 8)
DIRECT = ((2, 3), (2, 0))


def kernel(lab_hbm, wed_hbm, x_hbm, table_hbm, avg_ref, tot_ref,
           xo, xp, fo, fp, tb, wexp, lab, wed, lab_p, wed_p, slot_p, slot_w,
           s0, s1, s2, qs_0, qs_1, qs_2, q1_0, q1_1, q1_2, qd_0, qd_1, qd_2,
           qt_0, qt_1, qt_2, qf_0, qf_1, qf_2,
           sem_x, sem_t, sem_l, sem_ps, sem_pr, sem_ls, sem_lr,
           sem_s1, sem_s2, sem_r1, sem_rd, sem_rf):
    S = (s0, s1, s2)
    QS = (qs_0, qs_1, qs_2)
    Q1 = (q1_0, q1_1, q1_2)
    QD = (qd_0, qd_1, qd_2)
    QT = (qt_0, qt_1, qt_2)
    QF = (qf_0, qf_1, qf_2)
    y = lax.axis_index("cls")
    dom = lax.axis_index("dom")
    core = lax.rem(dom, 2)
    xc = lax.rem(dom // 2, 4)
    zc = dom // 8

    def device(dz=0, dx=0, dy=0, flip=False):
        c = 1 - core if flip else core
        zz, xx, yy = lax.rem(zc + dz, 4), lax.rem(xc + dx, 4), lax.rem(y + dy, 4)
        return (yy, (zz * 4 + xx) * 2 + c)

    def along(axis, step):
        return device(**{"d" + axis: step})

    partner = device(flip=True)
    barrier = pltpu.get_barrier_semaphore()
    peers = [partner] + [along(a, s) for a in "xyz" for s in (1, 3, 2)]
    for peer in peers:
        pl.semaphore_signal(barrier, inc=1, device_id=peer, device_id_type=MESH)

    def shard_of(pos, c):
        dz, dx = ORDER[pos]
        return (lax.rem(zc + dz, 4) * 4 + lax.rem(xc + dx, 4)) * 2 + c

    def window(pos, c):
        row = shard_of(pos, c) * (2 * NB)
        start = jnp.minimum(row // 8, (64 * NB - WINDOW) // 8) * 8
        return pl.multiple_of(start, 8), row - start

    def own_copy(pos):
        start, _ = window(pos, core)
        return pltpu.make_async_copy(
            x_hbm.at[:, pl.ds(start, WINDOW)], xo.at[pos], sem_x.at[pos // 4])

    def table_copy(pos):
        start = pl.multiple_of(shard_of(pos, core) * (NB * 128), 128)
        return pltpu.make_async_copy(
            table_hbm.at[:, pl.ds(start, NB * 128)], tb.at[pos], sem_t.at[pos // 4])

    def batch_of(pos):
        return BATCH[pos]

    def partner_copy(pos):
        start, _ = window(pos, 1 - core)
        return pltpu.make_async_remote_copy(
            src_ref=x_hbm.at[:, pl.ds(start, WINDOW)], dst_ref=xp.at[pos],
            send_sem=sem_ps, recv_sem=sem_pr.at[batch_of(pos)],
            device_id=partner, device_id_type=MESH)

    def wait_bytes(ref, sem):
        pltpu.make_async_copy(ref, ref, sem).wait()

    lab_local = pltpu.make_async_copy(lab_hbm, lab, sem_l.at[0])
    wed_local = pltpu.make_async_copy(wed_hbm, wed, sem_l.at[1])
    lab_local.start()
    wed_local.start()
    for pos in range(PIECES):
        table_copy(pos).start()
        own_copy(pos).start()
    pl.semaphore_wait(barrier, len(peers))

    lab_copy = pltpu.make_async_remote_copy(
        src_ref=lab_hbm, dst_ref=lab_p, send_sem=sem_ls.at[0], recv_sem=sem_lr.at[0],
        device_id=partner, device_id_type=MESH)
    wed_copy = pltpu.make_async_remote_copy(
        src_ref=wed_hbm, dst_ref=wed_p, send_sem=sem_ls.at[1], recv_sem=sem_lr.at[1],
        device_id=partner, device_id_type=MESH)
    lab_copy.start()
    wed_copy.start()
    for pos in range(PIECES):
        partner_copy(pos).start()

    def slots(lab_ref, wed_ref, base):
        labels = [lab_ref[p] for p in range(PDEV)]
        wedges = [wed_ref[p] for p in range(PDEV)]

        def one_class(k, carry):
            p1, w1, p2, w2 = 0, WEDGES, 0, WEDGES
            seen = jnp.int32(0)
            for p in range(PDEV):
                hit = labels[p] == k
                first = hit & (seen == 0)
                second = hit & (seen > 0)
                p1 = jnp.where(first, p, p1)
                w1 = jnp.where(first, wedges[p], w1)
                p2 = jnp.where(second, p, p2)
                w2 = jnp.where(second, wedges[p], w2)
                seen = seen + hit.astype(jnp.int32)
            slot_p[k * 4 + base] = p1
            slot_w[k * 4 + base] = w1
            slot_p[k * 4 + base + 1] = p2
            slot_w[k * 4 + base + 1] = w2
            return carry

        lax.fori_loop(0, 8, one_class, 0)

    lab_local.wait()
    wed_local.wait()
    slots(lab, wed, 0)

    def expand(piece):
        rows = wexp.at[piece].reshape((WEDGES + 1) * ROWS, 128)
        for b in range(NB):
            for lo, n in ((0, 8), (8, WEDGES - 8)):
                v = tb[piece, pl.ds(lo, n), pl.ds(b * 128, 128)]
                for c in range(2):
                    rows[pl.ds(lo * ROWS + 2 * b + c, n, stride=ROWS), :] = v
        wexp[piece, WEDGES] = jnp.zeros((ROWS, 128), F32)

    def unpack(src, dst, piece):
        def body(p, carry):
            dst[piece, p, pl.ds(0, WINDOW), :] = src[piece, p].astype(F32)
            return carry
        lax.fori_loop(0, PDEV, body, 0, unroll=True)

    for pos in range(PIECES):
        if pos % 4 == 0:
            wait_bytes(tb.at[pl.ds(pos, 4)], sem_t.at[pos // 4])
            wait_bytes(xo.at[pl.ds(pos, 4)], sem_x.at[pos // 4])
        expand(pos)
        unpack(xo, fo, pos)

    lab_copy.wait_recv()
    wed_copy.wait_recv()
    slots(lab_p, wed_p, 2)

    sub = lax.broadcasted_iota(jnp.int32, (TAIL, 128), 0)
    sub8 = lax.broadcasted_iota(jnp.int32, (8, 128), 0)
    lane8 = lax.broadcasted_iota(jnp.int32, (8, 128), 1)

    def chip_counts(dy):
        total = jnp.zeros((8, 128), F32)
        for j in range(2):
            k = lax.rem(y + dy, 4) * 2 + j
            for s in range(4):
                total = total + ((lane8 == slot_w[k * 4 + s]) & (sub8 == j)).astype(F32)
        return total

    def encode(dst, v, *more):
        n = v.shape[0]
        v = v.reshape(n // 8, 8, 128)
        top = jnp.maximum(jnp.max(jnp.abs(v), axis=0), 1e-30)
        code = jnp.ceil(jnp.log(top) * (STEPS / LN2))
        q = jnp.round(v * (jnp.exp(code * (-LN2 / STEPS)) * TOP)[None])
        rows = jnp.concatenate([q.reshape(n, 128), code, *more], axis=0)
        dst[...] = rows.astype(jnp.int32).astype(jnp.int16)

    def decode(src, n):
        rows = src[...].astype(jnp.int32).astype(F32)
        scale = jnp.exp(rows[n:n + 8] * (LN2 / STEPS)) * (1.0 / TOP)
        return (rows[0:n].reshape(n // 8, 8, 128) * scale[None]).reshape(n, 128), rows[n + 8:]

    def class_sum(piece, at, dy, j):
        dz, dx = ORDER[piece]
        k = lax.rem(y + dy, 4) * 2 + j
        total = None
        for s in range(4):
            p = slot_p[k * 4 + s]
            w = slot_w[k * 4 + s]
            src = fo if s < 2 else fp
            v = src[piece, p, pl.ds(at, ROWS), :] * wexp[piece, w]
            total = v if total is None else total + v
        tail = jnp.where(sub < TAIL - 2, total[HEAD:ROWS], 0.0)
        if j == 0:
            S[0][dx, dz, pl.ds(dy * HEAD, HEAD), :] = total[0:HEAD]
        else:
            S[1][dz, dx, pl.ds(dy * HEAD, HEAD), :] = total[0:HEAD]
        S[2][dy, dx, pl.ds(dz * 2 * TAIL + j * TAIL, TAIL), :] = tail

    def ring(t, src, dst, recv, step):
        return pltpu.make_async_remote_copy(
            src_ref=src, dst_ref=dst, send_sem=sem_s1.at[t], recv_sem=recv,
            device_id=along(AXES[t][0], step), device_id_type=MESH)

    def far1(t, rb):
        if (t, rb) in DIRECT:
            return ring(t, QS[t].at[rb], QD[t].at[rb, 2], sem_rd.at[t, rb], 2)
        return ring(t, QS[t].at[rb], Q1[t].at[rb], sem_r1.at[t, rb], 1 if rb >= 2 else 3)

    def own1(t, rb):
        side = 1 if rb >= 2 else 0
        return ring(t, QS[t].at[4 + rb], QD[t].at[rb, side], sem_rd.at[t, rb], 3 if side else 1)

    def comb1(t, rb):
        side = 0 if rb >= 2 else 1
        return ring(t, QS[t].at[8 + rb], QD[t].at[rb, side], sem_rd.at[t, rb], 3 if side else 1)

    def arrivals(t, rb):
        return 3 if (t, rb) in DIRECT else 2

    def plane(t, rb, rc):
        m = rb * 4 + rc - 1
        target = device(**{"d" + AXES[t][1]: rb, "d" + AXES[t][2]: rc})
        return pltpu.make_async_remote_copy(
            src_ref=QT[t].at[m], dst_ref=QF[t].at[m],
            send_sem=sem_s2.at[t], recv_sem=sem_rf.at[t],
            device_id=target, device_id_type=MESH)

    none = jnp.zeros((8, 128), F32)

    def counts_of(t, ra):
        return chip_counts(ra) if t == 2 else none

    def half(t, h):
        n = 2 * STREAM_ROWS[t]
        return pl.ds(h * n, n)

    def relay2(t, h):
        return copy(t, 12 + h, S[t].at[0, 2, half(t, h)], R2[t].at[half(t, h)], 1, 1 if h else 3)

    def own2(t, h):
        if h:
            return copy(t, 14 + h, S[t].at[0, 3, half(t, h)], EM[t].at[half(t, h)], 1, 3)
        return copy(t, 14 + h, S[t].at[0, 1, half(t, h)], EP[t].at[half(t, h)], 1, 1)

    def comb2(t, h):
        if h:
            return copy(t, 16 + h, S[t].at[0, 1, half(t, h)], EP[t].at[half(t, h)], 1, 1)
        return copy(t, 16 + h, S[t].at[0, 3, half(t, h)], EM[t].at[half(t, h)], 1, 3)

    def last3(t, rc):
        n = STREAM_ROWS[t]
        return copy(t, 17 + rc, S[t].at[0, 0, pl.ds(rc * n, n)], D3[t].at[rc - 1], 2, rc)

    done = set()
    sent = set()
    def column(rb):
        return [(d, rb) for d in range(4)]

    sends = ([(0, far1, rb, rb, 2, [(rb, 2)]) for rb in (2, 1, 3, 0)]
             + [(1, far1, rb, rb, 2, [(2, rb)]) for rb in (2, 1, 3, 0)]
             + [(2, far1, rb, rb, 2, column(rb)) for rb in (2, 1, 3, 0)]
             + [(0, own1, 4 + rb, rb, ra, [(rb, ra)]) for rb, ra in ((1, 1), (2, 3), (0, 1), (3, 3))]
             + [(1, own1, 4 + rb, rb, ra, [(ra, rb)]) for rb, ra in ((1, 1), (2, 3), (0, 1), (3, 3))]
             + [(2, own1, 4 + rb, rb, ra, column(rb)) for rb, ra in ((1, 1), (2, 3), (0, 1), (3, 3))]
             + [(t, comb1, 8 + rb, rb, 1 if rb >= 2 else 3, column(rb)) for t, rb in DIRECT])
    for pos in range(PIECES):
        if pos == 0 or batch_of(pos) != batch_of(pos - 1):
            batch = [p for p in range(PIECES) if batch_of(p) == batch_of(pos)]
            wait_bytes(xp.at[pl.ds(pos, len(batch))], sem_pr.at[batch_of(pos)])
        unpack(xp, fp, pos)
        at = window(pos, core)[1]

        def classes(dy, carry):
            for j in range(2):
                class_sum(pos, at, dy, j)
            return carry

        lax.fori_loop(0, 4, classes, 0)
        done.add(ORDER[pos])
        for i, (t, make, place, rb, ra, needs) in enumerate(sends):
            if i not in sent and done.issuperset(needs):
                sent.add(i)
                encode(QS[t].at[place], S[t][ra, rb], counts_of(t, ra))
                make(t, rb).start()

    for t, rb in ((0, 2), (1, 2), (0, 1), (1, 1), (2, 2), (0, 3), (1, 3), (0, 0), (1, 0), (2, 1)):
        far1(t, rb).wait_recv()
        ra = 1 if rb >= 2 else 3
        v, c = decode(Q1[t].at[rb], 4 * STREAM_ROWS[t])
        encode(QS[t].at[8 + rb], S[t][ra, rb] + v, counts_of(t, ra) + c)
        comb1(t, rb).start()
    kept = [None] * 3
    waited = set()

    def wait_ring(t, rb):
        if (t, rb) not in waited:
            waited.add((t, rb))
            wait_bytes(QD[t].at[rb, pl.ds(0, arrivals(t, rb))], sem_rd.at[t, rb])

    wait_ring(0, 2)
    wait_ring(1, 2)
    counts = None
    for t, rb in ((0, 2), (1, 2), (2, 3), (0, 1), (1, 1), (0, 3), (1, 3), (0, 0), (2, 0), (1, 0), (2, 2), (2, 1)):
        wait_ring(t, rb)
        r = STREAM_ROWS[t]
        total = S[t][0, rb]
        seen = chip_counts(0) if t == 2 else None
        for side in range(arrivals(t, rb)):
            v, c = decode(QD[t].at[rb, side], 4 * r)
            total = total + v
            if t == 2:
                seen = seen + c
        if t == 2 and counts is None:
            counts = seen
        more = (counts,) if t == 2 else ()
        for rc in (2, 1, 3, 0):
            part = total[rc * r:(rc + 1) * r]
            if rb or rc:
                encode(QT[t].at[rb * 4 + rc - 1], part, *more)
                plane(t, rb, rc).start()
            else:
                kept[t] = part
    final = []
    for t in (0, 1, 2):
        wait_bytes(QF[t], sem_rf.at[t])
        total = kept[t]
        for m in range(15):
            v, c = decode(QF[t].at[m], STREAM_ROWS[t])
            total = total + v
            if t == 2:
                counts = counts + c
        final.append(total)
    tail, heads = final[2], final[:2]

    counts_lane = lax.broadcasted_iota(jnp.int32, (1, 128), 1)
    even = lax.rem(lax.broadcasted_iota(jnp.int32, (ROWS, 128), 0), 2) == 0
    totals = []
    for j in range(2):
        row = counts[j:j + 1]
        total = jnp.zeros((ROWS, 128), F32)
        for w in range(WEDGES):
            n = jnp.sum(jnp.where(counts_lane == w, row, 0.0), axis=1, keepdims=True)
            a = wexp[PIECES - 1, w]
            total = total + n * (a * a)
        totals.append(total)
        summed = jnp.concatenate([heads[j], tail[j * TAIL:(j + 1) * TAIL]], axis=0)
        avg = summed / (total + 1.0)
        avg_ref[j] = avg[0:2 * NB].reshape(NB, 2, 128)
    tot_ref[...] = jnp.where(even, totals[0], totals[1])[0:2 * NB].reshape(NB, 2, 128)
    for t in range(3):
        wait_bytes(QS[t], sem_s1.at[t])
        wait_bytes(QT[t], sem_s2.at[t])
    wait_bytes(xp, sem_ps)
    lab_copy.wait_send()
    wed_copy.wait_send()


def put_out(avg_ref, tot_ref, avg_out, tot_out, sems):
    one = pltpu.make_async_copy(avg_ref, avg_out, sems.at[0])
    two = pltpu.make_async_copy(tot_ref, tot_out, sems.at[1])
    one.start()
    two.start()
    one.wait()
    two.wait()


def per_device(particles, labels, wedge_index, wedge_table):
    x = particles.reshape(PDEV, 2, 32 * NB, 128).transpose(0, 2, 1, 3)
    x = x.reshape(PDEV, 64 * NB, 128)
    lab = labels.reshape(PDEV)
    hbm = pl.BlockSpec(memory_space=pltpu.HBM)
    vmem = pl.BlockSpec(memory_space=pltpu.VMEM)
    dma = pltpu.SemaphoreType.DMA
    V = pltpu.VMEM

    def per_stream(*lead):
        return [V((*lead, 4 * r, 128), F32) for r in STREAM_ROWS]

    def coded(*lead):
        return [V((*lead, 4 * r + 16, 128), jnp.int16) for r in STREAM_ROWS]

    shapes = (jax.ShapeDtypeStruct((2, NB, 2, 128), F32),
              jax.ShapeDtypeStruct((NB, 2, 128), F32))
    avg, tot = pl.pallas_call(
        kernel,
        out_shape=shapes,
        in_specs=[hbm] * 4,
        out_specs=(vmem, vmem),
        scratch_shapes=[
            V((PIECES, PDEV, WINDOW, 128), BF16),
            V((PIECES, PDEV, WINDOW, 128), BF16),
            V((PIECES, PDEV, WINDOW + 8, 128), F32),
            V((PIECES, PDEV, WINDOW + 8, 128), F32),
            V((PIECES, WEDGES, NB * 128), F32),
            V((PIECES, WEDGES + 1, ROWS, 128), F32),
            *[pltpu.SMEM((PDEV,), jnp.int32)] * 4,
            pltpu.SMEM((32,), jnp.int32),
            pltpu.SMEM((32,), jnp.int32),
            *per_stream(4, 4),
            *coded(12), *coded(4), *coded(4, 3),
            *[V((15, HEAD + 8, 128), jnp.int16)] * 6,
            dma((4,)), dma((4,)), dma((2,)), dma(()), dma((9,)), dma((2,)), dma((2,)),
            dma((3,)), dma((3,)), dma((3, 4)), dma((3, 4)), dma((3,)),
        ],
        compiler_params=pltpu.CompilerParams(
            collective_id=0, has_side_effects=True, vmem_limit_bytes=44 * 1024 * 1024),
        name="class_sums",
    )(*[pltpu.with_memory_space_constraint(a, pltpu.HBM) for a in (lab, wedge_index, x, wedge_table)])
    avg, tot = pl.pallas_call(
        put_out,
        out_shape=shapes,
        in_specs=[vmem] * 2,
        out_specs=(hbm, hbm),
        scratch_shapes=[dma((2,))],
        compiler_params=pltpu.CompilerParams(vmem_limit_bytes=1024 * 1024),
        name="put_out",
    )(avg, tot)
    avg = avg.transpose(0, 2, 1, 3).reshape(2, 2, NB * 128)
    tot = tot.transpose(1, 0, 2).reshape(2, NB * 128)
    return avg, tot


def solution(mesh):
    return jax.shard_map(
        per_device,
        mesh=mesh,
        in_specs=(P(("cls", "dom"), None, None), P(("cls", "dom"), None), P(("cls", "dom")), P()),
        out_specs=(P("cls", None, "dom"), P("cls", "dom")),
        check_vma=False,
    )
```

```python
import jax
import jax.numpy as jnp
from jax import lax
from jax.experimental import pallas as pl
from jax.experimental.pallas import tpu as pltpu
from jax.sharding import PartitionSpec as P

F32 = jnp.float32
BF16 = jnp.bfloat16
MESH = pl.DeviceIdType.MESH
NB = 27
ROWS = 56
WEDGES = 12
PDEV = 8
PIECES = 16
HEAD = 40
TAIL = ROWS - HEAD
STREAM_ROWS = (HEAD, HEAD, 2 * TAIL)
WINDOW = 64
WROWS = 72
EMPTY = 10000
TOP = 32700.0
STEPS = 64.0
LN2 = 0.6931471805599453
AXES = (("x", "z", "y"), ("z", "x", "y"), ("y", "x", "z"))
ORDER = ((2, 2), (1, 2), (2, 1), (3, 2), (2, 3), (0, 2), (2, 0), (1, 1),
         (0, 1), (3, 1), (3, 3), (1, 3), (0, 3), (1, 0), (3, 0), (0, 0))
BATCH = (0, 1, 2, 3, 4, 5, 5, 6, 6, 6, 7, 7, 7, 8, 8, 8)
HOLD = 7
DIRECT = ((2, 3), (2, 0))


def kernel(lab_hbm, wed_hbm, x_hbm, table_hbm, avg_ref, tot_ref,
           xo, xp, prod, tb, wexp, lab, wed, lab_p, wed_p, slot_p, slot_w,
           s0, s1, s2, qs_0, qs_1, qs_2, q1_0, q1_1, q1_2, qd_0, qd_1, qd_2,
           qt_0, qt_1, qt_2, qf_0, qf_1, qf_2,
           sem_x, sem_t, sem_l, sem_ps, sem_pr, sem_ls, sem_lr,
           sem_s1, sem_s2, sem_r1, sem_rd, sem_rf):
    S = (s0, s1, s2)
    QS = (qs_0, qs_1, qs_2)
    Q1 = (q1_0, q1_1, q1_2)
    QD = (qd_0, qd_1, qd_2)
    QT = (qt_0, qt_1, qt_2)
    QF = (qf_0, qf_1, qf_2)
    y = lax.axis_index("cls")
    dom = lax.axis_index("dom")
    core = lax.rem(dom, 2)
    xc = lax.rem(dom // 2, 4)
    zc = dom // 8

    def device(dz=0, dx=0, dy=0, flip=False):
        c = 1 - core if flip else core
        zz, xx, yy = lax.rem(zc + dz, 4), lax.rem(xc + dx, 4), lax.rem(y + dy, 4)
        return (yy, (zz * 4 + xx) * 2 + c)

    def along(axis, step):
        return device(**{"d" + axis: step})

    partner = device(flip=True)
    barrier = pltpu.get_barrier_semaphore()
    peers = [partner] + [along(a, s) for a in "xyz" for s in (1, 3, 2)]
    for peer in peers:
        pl.semaphore_signal(barrier, inc=1, device_id=peer, device_id_type=MESH)

    def shard_of(pos, c):
        dz, dx = ORDER[pos]
        return (lax.rem(zc + dz, 4) * 4 + lax.rem(xc + dx, 4)) * 2 + c

    def window(pos, c):
        row = shard_of(pos, c) * (2 * NB)
        start = jnp.minimum(row // 8, (64 * NB - WINDOW) // 8) * 8
        return pl.multiple_of(start, 8), row - start

    def own_copy(pos):
        start, _ = window(pos, core)
        return pltpu.make_async_copy(
            x_hbm.at[:, pl.ds(start, WINDOW)], xo.at[pos], sem_x.at[pos // 4])

    def table_copy(pos):
        start = pl.multiple_of(shard_of(pos, core) * (NB * 128), 128)
        return pltpu.make_async_copy(
            table_hbm.at[:, pl.ds(start, NB * 128)], tb.at[pos], sem_t.at[pos // 4])

    def batch_of(pos):
        return BATCH[pos]

    def partner_copy(pos):
        start, _ = window(pos, 1 - core)
        return pltpu.make_async_remote_copy(
            src_ref=x_hbm.at[:, pl.ds(start, WINDOW)], dst_ref=xp.at[pos],
            send_sem=sem_ps, recv_sem=sem_pr.at[batch_of(pos)],
            device_id=partner, device_id_type=MESH)

    def wait_bytes(ref, sem):
        pltpu.make_async_copy(ref, ref, sem).wait()

    lab_local = pltpu.make_async_copy(lab_hbm, lab, sem_l.at[0])
    wed_local = pltpu.make_async_copy(wed_hbm, wed, sem_l.at[1])
    lab_local.start()
    wed_local.start()
    for pos in range(PIECES):
        table_copy(pos).start()
        own_copy(pos).start()
    pl.semaphore_wait(barrier, len(peers))

    lab_copy = pltpu.make_async_remote_copy(
        src_ref=lab_hbm, dst_ref=lab_p, send_sem=sem_ls.at[0], recv_sem=sem_lr.at[0],
        device_id=partner, device_id_type=MESH)
    wed_copy = pltpu.make_async_remote_copy(
        src_ref=wed_hbm, dst_ref=wed_p, send_sem=sem_ls.at[1], recv_sem=sem_lr.at[1],
        device_id=partner, device_id_type=MESH)
    lab_copy.start()
    wed_copy.start()
    for pos in range(PIECES):
        partner_copy(pos).start()

    def slots(lab_ref, wed_ref, base):
        labels = [lab_ref[p] for p in range(PDEV)]
        wedges = [wed_ref[p] for p in range(PDEV)]

        def one_class(k, carry):
            p1, w1, p2, w2 = EMPTY, WEDGES, EMPTY, WEDGES
            seen = jnp.int32(0)
            for p in range(PDEV):
                hit = labels[p] == k
                first = hit & (seen == 0)
                second = hit & (seen > 0)
                p1 = jnp.where(first, base * 4 + p, p1)
                w1 = jnp.where(first, wedges[p], w1)
                p2 = jnp.where(second, base * 4 + p, p2)
                w2 = jnp.where(second, wedges[p], w2)
                seen = seen + hit.astype(jnp.int32)
            slot_p[k * 4 + base] = p1
            slot_w[k * 4 + base] = w1
            slot_p[k * 4 + base + 1] = p2
            slot_w[k * 4 + base + 1] = w2
            return carry

        lax.fori_loop(0, 8, one_class, 0)

    lab_local.wait()
    wed_local.wait()
    slots(lab, wed, 0)

    def expand(pos):
        rows = wexp.at[pos].reshape(WEDGES * WROWS, 128)
        at = window(pos, core)[1]
        for b in range(NB):
            for lo, n in ((0, 8), (8, WEDGES - 8)):
                v = tb[pos, pl.ds(lo, n), pl.ds(b * 128, 128)]
                for c in range(2):
                    rows[pl.ds(at + lo * WROWS + 2 * b + c, n, stride=WROWS), :] = v

    def weigh(src, wedges, base, pos):
        for p in range(PDEV):
            prod[pos * 16 + base + p, pl.ds(0, WINDOW), :] = (
                src[pos, p].astype(F32) * wexp[pos, wedges[p], pl.ds(0, WINDOW), :])

    prod[PIECES * 16] = jnp.zeros((WROWS, 128), F32)

    for pos in range(PIECES):
        if pos % 4 == 0:
            wait_bytes(tb.at[pl.ds(pos, 4)], sem_t.at[pos // 4])
            wait_bytes(xo.at[pl.ds(pos, 4)], sem_x.at[pos // 4])
        expand(pos)
        weigh(xo, wed, 0, pos)

    lab_copy.wait_recv()
    wed_copy.wait_recv()
    slots(lab_p, wed_p, 2)

    sub = lax.broadcasted_iota(jnp.int32, (TAIL, 128), 0)
    sub8 = lax.broadcasted_iota(jnp.int32, (8, 128), 0)
    lane8 = lax.broadcasted_iota(jnp.int32, (8, 128), 1)

    def chip_counts(dy):
        total = jnp.zeros((8, 128), F32)
        for j in range(2):
            k = lax.rem(y + dy, 4) * 2 + j
            for s in range(4):
                total = total + ((lane8 == slot_w[k * 4 + s]) & (sub8 == j)).astype(F32)
        return total

    def encode(dst, v, *more):
        n = v.shape[0]
        v = v.reshape(n // 8, 8, 128)
        top = jnp.maximum(jnp.max(jnp.abs(v), axis=0), 1e-30)
        code = jnp.ceil(jnp.log(top) * (STEPS / LN2))
        q = jnp.round(v * (jnp.exp(code * (-LN2 / STEPS)) * TOP)[None])
        rows = jnp.concatenate([q.reshape(n, 128), code, *more], axis=0)
        dst[...] = rows.astype(jnp.int32).astype(jnp.int16)

    def decode(src, n):
        rows = src[...].astype(jnp.int32).astype(F32)
        scale = jnp.exp(rows[n:n + 8] * (LN2 / STEPS)) * (1.0 / TOP)
        return (rows[0:n].reshape(n // 8, 8, 128) * scale[None]).reshape(n, 128), rows[n + 8:]

    def class_sum(piece, at, dy, j):
        dz, dx = ORDER[piece]
        k = lax.rem(y + dy, 4) * 2 + j
        total = None
        for s in range(4):
            place = jnp.minimum(slot_p[k * 4 + s] + piece * 16, PIECES * 16)
            v = prod[place, pl.ds(at, ROWS), :]
            total = v if total is None else total + v
        tail = jnp.where(sub < TAIL - 2, total[HEAD:ROWS], 0.0)
        if j == 0:
            S[0][dx, dz, pl.ds(dy * HEAD, HEAD), :] = total[0:HEAD]
        else:
            S[1][dz, dx, pl.ds(dy * HEAD, HEAD), :] = total[0:HEAD]
        S[2][dy, dx, pl.ds(dz * 2 * TAIL + j * TAIL, TAIL), :] = tail

    def ring(t, src, dst, recv, step):
        return pltpu.make_async_remote_copy(
            src_ref=src, dst_ref=dst, send_sem=sem_s1.at[t], recv_sem=recv,
            device_id=along(AXES[t][0], step), device_id_type=MESH)

    def far1(t, rb):
        if (t, rb) in DIRECT:
            return ring(t, QS[t].at[rb], QD[t].at[rb, 2], sem_rd.at[t, rb], 2)
        return ring(t, QS[t].at[rb], Q1[t].at[rb], sem_r1.at[t, rb], 1 if rb >= 2 else 3)

    def own1(t, rb):
        side = 1 if rb >= 2 else 0
        return ring(t, QS[t].at[4 + rb], QD[t].at[rb, side], sem_rd.at[t, rb], 3 if side else 1)

    def comb1(t, rb):
        side = 0 if rb >= 2 else 1
        return ring(t, QS[t].at[8 + rb], QD[t].at[rb, side], sem_rd.at[t, rb], 3 if side else 1)

    def arrivals(t, rb):
        return 3 if (t, rb) in DIRECT else 2

    def plane(t, rb, rc):
        m = rb * 4 + rc - 1
        target = device(**{"d" + AXES[t][1]: rb, "d" + AXES[t][2]: rc})
        return pltpu.make_async_remote_copy(
            src_ref=QT[t].at[m], dst_ref=QF[t].at[m],
            send_sem=sem_s2.at[t], recv_sem=sem_rf.at[t],
            device_id=target, device_id_type=MESH)

    def counts_of(t, ra):
        return (chip_counts(ra),) if t == 2 else ()

    def half(t, h):
        n = 2 * STREAM_ROWS[t]
        return pl.ds(h * n, n)

    def relay2(t, h):
        return copy(t, 12 + h, S[t].at[0, 2, half(t, h)], R2[t].at[half(t, h)], 1, 1 if h else 3)

    def own2(t, h):
        if h:
            return copy(t, 14 + h, S[t].at[0, 3, half(t, h)], EM[t].at[half(t, h)], 1, 3)
        return copy(t, 14 + h, S[t].at[0, 1, half(t, h)], EP[t].at[half(t, h)], 1, 1)

    def comb2(t, h):
        if h:
            return copy(t, 16 + h, S[t].at[0, 1, half(t, h)], EP[t].at[half(t, h)], 1, 1)
        return copy(t, 16 + h, S[t].at[0, 3, half(t, h)], EM[t].at[half(t, h)], 1, 3)

    def last3(t, rc):
        n = STREAM_ROWS[t]
        return copy(t, 17 + rc, S[t].at[0, 0, pl.ds(rc * n, n)], D3[t].at[rc - 1], 2, rc)

    done = set()
    held = []
    sent = set()
    def column(rb):
        return [(d, rb) for d in range(4)]

    sends = ([(0, far1, rb, rb, 2, [(rb, 2)]) for rb in (2, 1, 3, 0)]
             + [(1, far1, rb, rb, 2, [(2, rb)]) for rb in (2, 1, 3, 0)]
             + [(2, far1, rb, rb, 2, column(rb)) for rb in (2, 1, 3, 0)]
             + [(0, own1, 4 + rb, rb, ra, [(rb, ra)]) for rb, ra in ((1, 1), (2, 3), (0, 1), (3, 3))]
             + [(1, own1, 4 + rb, rb, ra, [(ra, rb)]) for rb, ra in ((1, 1), (2, 3), (0, 1), (3, 3))]
             + [(2, own1, 4 + rb, rb, ra, column(rb)) for rb, ra in ((1, 1), (2, 3), (0, 1), (3, 3))]
             + [(t, comb1, 8 + rb, rb, 1 if rb >= 2 else 3, column(rb)) for t, rb in DIRECT])
    for pos in range(PIECES):
        if pos == 0 or batch_of(pos) != batch_of(pos - 1):
            batch = [p for p in range(PIECES) if batch_of(p) == batch_of(pos)]
            wait_bytes(xp.at[pl.ds(pos, len(batch))], sem_pr.at[batch_of(pos)])
        weigh(xp, wed_p, 8, pos)
        at = window(pos, core)[1]

        def classes(dy, carry):
            for j in range(2):
                class_sum(pos, at, dy, j)
            return carry

        lax.fori_loop(0, 4, classes, 0)
        done.add(ORDER[pos])
        for i, (t, make, place, rb, ra, needs) in enumerate(sends):
            if i not in sent and done.issuperset(needs):
                sent.add(i)
                encode(QS[t].at[place], S[t][ra, rb], *counts_of(t, ra))
                if make is own1 and pos < HOLD:
                    held.append((t, rb))
                else:
                    make(t, rb).start()
        if pos == HOLD:
            for t, rb in held:
                own1(t, rb).start()

    for t, rb in ((0, 2), (1, 2), (0, 1), (1, 1), (0, 3), (2, 2), (1, 3), (0, 0), (1, 0), (2, 1)):
        far1(t, rb).wait_recv()
        ra = 1 if rb >= 2 else 3
        v, c = decode(Q1[t].at[rb], 4 * STREAM_ROWS[t])
        encode(QS[t].at[8 + rb], S[t][ra, rb] + v, *[n + c for n in counts_of(t, ra)])
        comb1(t, rb).start()
    kept = [None] * 3
    waited = set()

    def wait_ring(t, rb):
        if (t, rb) not in waited:
            waited.add((t, rb))
            wait_bytes(QD[t].at[rb, pl.ds(0, arrivals(t, rb))], sem_rd.at[t, rb])

    wait_ring(0, 2)
    wait_ring(1, 2)
    counts = None
    for t, rb in ((0, 2), (1, 2), (2, 3), (0, 1), (1, 1), (2, 2), (2, 1), (0, 3), (1, 3), (0, 0), (2, 0), (1, 0)):
        wait_ring(t, rb)
        r = STREAM_ROWS[t]
        total = S[t][0, rb]
        seen = chip_counts(0) if t == 2 else None
        for side in range(arrivals(t, rb)):
            v, c = decode(QD[t].at[rb, side], 4 * r)
            total = total + v
            if t == 2:
                seen = seen + c
        if t == 2 and counts is None:
            counts = seen
        more = (counts,) if t == 2 else ()
        for rc in (2, 1, 3, 0):
            part = total[rc * r:(rc + 1) * r]
            if rb or rc:
                encode(QT[t].at[rb * 4 + rc - 1], part, *more)
                plane(t, rb, rc).start()
            else:
                kept[t] = part
    final = []
    for t in (0, 1, 2):
        wait_bytes(QF[t], sem_rf.at[t])
        total = kept[t]
        for m in range(15):
            v, c = decode(QF[t].at[m], STREAM_ROWS[t])
            total = total + v
            if t == 2:
                counts = counts + c
        final.append(total)
    tail, heads = final[2], final[:2]

    counts_lane = lax.broadcasted_iota(jnp.int32, (1, 128), 1)
    even = lax.rem(lax.broadcasted_iota(jnp.int32, (ROWS, 128), 0), 2) == 0
    own_at = window(PIECES - 1, core)[1]
    totals = []
    for j in range(2):
        row = counts[j:j + 1]
        total = jnp.zeros((ROWS, 128), F32)
        for w in range(WEDGES):
            n = jnp.sum(jnp.where(counts_lane == w, row, 0.0), axis=1, keepdims=True)
            a = wexp[PIECES - 1, w, pl.ds(own_at, ROWS), :]
            total = total + n * (a * a)
        totals.append(total)
        summed = jnp.concatenate([heads[j], tail[j * TAIL:(j + 1) * TAIL]], axis=0)
        avg = summed / (total + 1.0)
        avg_ref[j] = avg[0:2 * NB].reshape(NB, 2, 128)
    tot_ref[...] = jnp.where(even, totals[0], totals[1])[0:2 * NB].reshape(NB, 2, 128)
    for t in range(3):
        wait_bytes(QS[t], sem_s1.at[t])
        wait_bytes(QT[t], sem_s2.at[t])
    wait_bytes(xp, sem_ps)
    lab_copy.wait_send()
    wed_copy.wait_send()


def put_out(avg_ref, tot_ref, avg_out, tot_out, sems):
    one = pltpu.make_async_copy(avg_ref, avg_out, sems.at[0])
    two = pltpu.make_async_copy(tot_ref, tot_out, sems.at[1])
    one.start()
    two.start()
    one.wait()
    two.wait()


def per_device(particles, labels, wedge_index, wedge_table):
    x = particles.reshape(PDEV, 2, 32 * NB, 128).transpose(0, 2, 1, 3)
    x = x.reshape(PDEV, 64 * NB, 128)
    lab = labels.reshape(PDEV)
    hbm = pl.BlockSpec(memory_space=pltpu.HBM)
    vmem = pl.BlockSpec(memory_space=pltpu.VMEM)
    dma = pltpu.SemaphoreType.DMA
    V = pltpu.VMEM

    def per_stream(*lead):
        return [V((*lead, 4 * r, 128), F32) for r in STREAM_ROWS]

    def coded(*lead):
        return [V((*lead, 4 * r + extra, 128), jnp.int16)
                for r, extra in zip(STREAM_ROWS, (8, 8, 16))]

    shapes = (jax.ShapeDtypeStruct((2, NB, 2, 128), F32),
              jax.ShapeDtypeStruct((NB, 2, 128), F32))
    avg, tot = pl.pallas_call(
        kernel,
        out_shape=shapes,
        in_specs=[hbm] * 4,
        out_specs=(vmem, vmem),
        scratch_shapes=[
            V((PIECES, PDEV, WINDOW, 128), BF16),
            V((PIECES, PDEV, WINDOW, 128), BF16),
            V((PIECES * 16 + 1, WROWS, 128), F32),
            V((PIECES, WEDGES, NB * 128), F32),
            V((PIECES, WEDGES, WROWS, 128), F32),
            *[pltpu.SMEM((PDEV,), jnp.int32)] * 4,
            pltpu.SMEM((32,), jnp.int32),
            pltpu.SMEM((32,), jnp.int32),
            *per_stream(4, 4),
            *coded(12), *coded(4), *coded(4, 3),
            *[V((15, HEAD + 8, 128), jnp.int16)] * 6,
            dma((4,)), dma((4,)), dma((2,)), dma(()), dma((9,)), dma((2,)), dma((2,)),
            dma((3,)), dma((3,)), dma((3, 4)), dma((3, 4)), dma((3,)),
        ],
        compiler_params=pltpu.CompilerParams(
            collective_id=0, has_side_effects=True, vmem_limit_bytes=44 * 1024 * 1024),
        name="class_sums",
    )(*[pltpu.with_memory_space_constraint(a, pltpu.HBM) for a in (lab, wedge_index, x, wedge_table)])
    avg, tot = pl.pallas_call(
        put_out,
        out_shape=shapes,
        in_specs=[vmem] * 2,
        out_specs=(hbm, hbm),
        scratch_shapes=[dma((2,))],
        compiler_params=pltpu.CompilerParams(vmem_limit_bytes=1024 * 1024),
        name="put_out",
    )(avg, tot)
    avg = avg.transpose(0, 2, 1, 3).reshape(2, 2, NB * 128)
    tot = tot.transpose(1, 0, 2).reshape(2, NB * 128)
    return avg, tot


def solution(mesh):
    return jax.shard_map(
        per_device,
        mesh=mesh,
        in_specs=(P(("cls", "dom"), None, None), P(("cls", "dom"), None), P(("cls", "dom")), P()),
        out_specs=(P("cls", None, "dom"), P("cls", "dom")),
        check_vma=False,
    )
```

```python
import jax
import jax.numpy as jnp
from jax import lax
from jax.experimental import pallas as pl
from jax.experimental.pallas import tpu as pltpu
from jax.sharding import PartitionSpec as P

F32 = jnp.float32
BF16 = jnp.bfloat16
MESH = pl.DeviceIdType.MESH
NB = 27
ROWS = 56
WEDGES = 12
PDEV = 8
PIECES = 16
HEAD = 40
TAIL = ROWS - HEAD
STREAM_ROWS = (HEAD, HEAD, 2 * TAIL)
WINDOW = 64
WROWS = 72
EMPTY = 10000
TOP = 32700.0
STEPS = 64.0
LN2 = 0.6931471805599453
AXES = (("x", "z", "y"), ("z", "x", "y"), ("y", "x", "z"))
ORDER = ((2, 2), (1, 2), (2, 1), (3, 2), (2, 3), (0, 2), (2, 0), (1, 1),
         (0, 1), (3, 1), (3, 3), (1, 3), (0, 3), (1, 0), (3, 0), (0, 0))
BATCH = (0, 1, 2, 3, 4, 5, 5, 6, 6, 6, 7, 7, 7, 8, 8, 8)
HOLD = 7
DIRECT = ((2, 3), (2, 0))


def kernel(lab_hbm, wed_hbm, x_hbm, table_hbm, avg_ref, tot_ref,
           xo, xp, prod, tb, wexp, lab, wed, lab_p, wed_p, slot_p, slot_w,
           s0, s1, s2, qs_0, qs_1, qs_2, q1_0, q1_1, q1_2, qd_0, qd_1, qd_2,
           qt_0, qt_1, qt_2, qf_0, qf_1, qf_2,
           sem_x, sem_t, sem_l, sem_ps, sem_pr, sem_ls, sem_lr,
           sem_s1, sem_s2, sem_r1, sem_rd, sem_rf):
    S = (s0, s1, s2)
    QS = (qs_0, qs_1, qs_2)
    Q1 = (q1_0, q1_1, q1_2)
    QD = (qd_0, qd_1, qd_2)
    QT = (qt_0, qt_1, qt_2)
    QF = (qf_0, qf_1, qf_2)
    y = lax.axis_index("cls")
    dom = lax.axis_index("dom")
    core = lax.rem(dom, 2)
    xc = lax.rem(dom // 2, 4)
    zc = dom // 8

    def device(dz=0, dx=0, dy=0, flip=False):
        c = 1 - core if flip else core
        zz, xx, yy = lax.rem(zc + dz, 4), lax.rem(xc + dx, 4), lax.rem(y + dy, 4)
        return (yy, (zz * 4 + xx) * 2 + c)

    def along(axis, step):
        return device(**{"d" + axis: step})

    partner = device(flip=True)
    barrier = pltpu.get_barrier_semaphore()
    peers = [partner] + [along(a, s) for a in "xyz" for s in (1, 3, 2)]
    for peer in peers:
        pl.semaphore_signal(barrier, inc=1, device_id=peer, device_id_type=MESH)

    def shard_of(pos, c):
        dz, dx = ORDER[pos]
        return (lax.rem(zc + dz, 4) * 4 + lax.rem(xc + dx, 4)) * 2 + c

    def window(pos, c):
        row = shard_of(pos, c) * (2 * NB)
        start = jnp.minimum(row // 8, (64 * NB - WINDOW) // 8) * 8
        return pl.multiple_of(start, 8), row - start

    def own_copy(pos):
        start, _ = window(pos, core)
        return pltpu.make_async_copy(
            x_hbm.at[:, pl.ds(start, WINDOW)], xo.at[pos], sem_x.at[pos // 4])

    def table_copy(pos):
        start = pl.multiple_of(shard_of(pos, core) * (NB * 128), 128)
        return pltpu.make_async_copy(
            table_hbm.at[:, pl.ds(start, NB * 128)], tb.at[pos], sem_t.at[pos // 4])

    def batch_of(pos):
        return BATCH[pos]

    def partner_copy(pos):
        start, _ = window(pos, 1 - core)
        return pltpu.make_async_remote_copy(
            src_ref=x_hbm.at[:, pl.ds(start, WINDOW)], dst_ref=xp.at[pos],
            send_sem=sem_ps, recv_sem=sem_pr.at[batch_of(pos)],
            device_id=partner, device_id_type=MESH)

    def wait_bytes(ref, sem):
        pltpu.make_async_copy(ref, ref, sem).wait()

    lab_local = pltpu.make_async_copy(lab_hbm, lab, sem_l.at[0])
    wed_local = pltpu.make_async_copy(wed_hbm, wed, sem_l.at[1])
    lab_local.start()
    wed_local.start()
    for pos in range(PIECES):
        table_copy(pos).start()
        own_copy(pos).start()
    pl.semaphore_wait(barrier, len(peers))

    lab_copy = pltpu.make_async_remote_copy(
        src_ref=lab_hbm, dst_ref=lab_p, send_sem=sem_ls.at[0], recv_sem=sem_lr.at[0],
        device_id=partner, device_id_type=MESH)
    wed_copy = pltpu.make_async_remote_copy(
        src_ref=wed_hbm, dst_ref=wed_p, send_sem=sem_ls.at[1], recv_sem=sem_lr.at[1],
        device_id=partner, device_id_type=MESH)
    lab_copy.start()
    wed_copy.start()
    for pos in range(PIECES):
        partner_copy(pos).start()

    def slots(lab_ref, wed_ref, base):
        labels = [lab_ref[p] for p in range(PDEV)]
        wedges = [wed_ref[p] for p in range(PDEV)]

        def one_class(k, carry):
            p1, w1, p2, w2 = EMPTY, WEDGES, EMPTY, WEDGES
            seen = jnp.int32(0)
            for p in range(PDEV):
                hit = labels[p] == k
                first = hit & (seen == 0)
                second = hit & (seen > 0)
                p1 = jnp.where(first, base * 4 + p, p1)
                w1 = jnp.where(first, wedges[p], w1)
                p2 = jnp.where(second, base * 4 + p, p2)
                w2 = jnp.where(second, wedges[p], w2)
                seen = seen + hit.astype(jnp.int32)
            slot_p[k * 4 + base] = p1
            slot_w[k * 4 + base] = w1
            slot_p[k * 4 + base + 1] = p2
            slot_w[k * 4 + base + 1] = w2
            return carry

        lax.fori_loop(0, 8, one_class, 0)

    lab_local.wait()
    wed_local.wait()
    slots(lab, wed, 0)

    def expand(pos):
        rows = wexp.at[pos].reshape(WEDGES * WROWS, 128)
        at = window(pos, core)[1]
        for b in range(NB):
            for lo, n in ((0, 8), (8, WEDGES - 8)):
                v = tb[pos, pl.ds(lo, n), pl.ds(b * 128, 128)]
                for c in range(2):
                    rows[pl.ds(at + lo * WROWS + 2 * b + c, n, stride=WROWS), :] = v

    def weigh(src, wedges, base, pos):
        for p in range(PDEV):
            prod[pos * 16 + base + p, pl.ds(0, WINDOW), :] = (
                src[pos, p].astype(F32) * wexp[pos, wedges[p], pl.ds(0, WINDOW), :])

    prod[PIECES * 16] = jnp.zeros((WROWS, 128), F32)

    for pos in range(PIECES):
        if pos % 4 == 0:
            wait_bytes(tb.at[pl.ds(pos, 4)], sem_t.at[pos // 4])
            wait_bytes(xo.at[pl.ds(pos, 4)], sem_x.at[pos // 4])
        expand(pos)
        weigh(xo, wed, 0, pos)

    lab_copy.wait_recv()
    wed_copy.wait_recv()
    slots(lab_p, wed_p, 2)

    sub = lax.broadcasted_iota(jnp.int32, (TAIL, 128), 0)
    sub8 = lax.broadcasted_iota(jnp.int32, (8, 128), 0)
    lane8 = lax.broadcasted_iota(jnp.int32, (8, 128), 1)

    def chip_counts(dy):
        total = jnp.zeros((8, 128), F32)
        for j in range(2):
            k = lax.rem(y + dy, 4) * 2 + j
            for s in range(4):
                total = total + ((lane8 == slot_w[k * 4 + s]) & (sub8 == j)).astype(F32)
        return total

    def encode(dst, v, *more):
        n = v.shape[0]
        v = v.reshape(n // 8, 8, 128)
        top = jnp.maximum(jnp.max(jnp.abs(v), axis=0), 1e-30)
        code = jnp.ceil(jnp.log(top) * (STEPS / LN2))
        q = jnp.round(v * (jnp.exp(code * (-LN2 / STEPS)) * TOP)[None])
        rows = jnp.concatenate([q.reshape(n, 128), code, *more], axis=0)
        dst[...] = rows.astype(jnp.int32).astype(jnp.int16)

    def decode(src, n):
        rows = src[...].astype(jnp.int32).astype(F32)
        scale = jnp.exp(rows[n:n + 8] * (LN2 / STEPS)) * (1.0 / TOP)
        return (rows[0:n].reshape(n // 8, 8, 128) * scale[None]).reshape(n, 128), rows[n + 8:]

    def class_sum(piece, at, dy, j):
        dz, dx = ORDER[piece]
        k = lax.rem(y + dy, 4) * 2 + j
        total = None
        for s in range(4):
            place = jnp.minimum(slot_p[k * 4 + s] + piece * 16, PIECES * 16)
            v = prod[place, pl.ds(at, ROWS), :]
            total = v if total is None else total + v
        tail = jnp.where(sub < TAIL - 2, total[HEAD:ROWS], 0.0)
        if j == 0:
            S[0][dx, dz, pl.ds(dy * HEAD, HEAD), :] = total[0:HEAD]
        else:
            S[1][dz, dx, pl.ds(dy * HEAD, HEAD), :] = total[0:HEAD]
        S[2][dy, dx, pl.ds(dz * 2 * TAIL + j * TAIL, TAIL), :] = tail

    def ring(t, src, dst, recv, step):
        return pltpu.make_async_remote_copy(
            src_ref=src, dst_ref=dst, send_sem=sem_s1.at[t], recv_sem=recv,
            device_id=along(AXES[t][0], step), device_id_type=MESH)

    def far1(t, rb):
        if (t, rb) in DIRECT:
            return ring(t, QS[t].at[rb], QD[t].at[rb, 2], sem_rd.at[t, rb], 2)
        return ring(t, QS[t].at[rb], Q1[t].at[rb], sem_r1.at[t, rb], 1 if rb >= 2 else 3)

    def own1(t, rb):
        side = 1 if rb >= 2 else 0
        return ring(t, QS[t].at[4 + rb], QD[t].at[rb, side], sem_rd.at[t, rb], 3 if side else 1)

    def comb1(t, rb):
        side = 0 if rb >= 2 else 1
        return ring(t, QS[t].at[8 + rb], QD[t].at[rb, side], sem_rd.at[t, rb], 3 if side else 1)

    def arrivals(t, rb):
        return 3 if (t, rb) in DIRECT else 2

    def plane(t, rb, rc):
        m = rb * 4 + rc - 1
        target = device(**{"d" + AXES[t][1]: rb, "d" + AXES[t][2]: rc})
        return pltpu.make_async_remote_copy(
            src_ref=QT[t].at[m], dst_ref=QF[t].at[m],
            send_sem=sem_s2.at[t], recv_sem=sem_rf.at[t],
            device_id=target, device_id_type=MESH)

    def counts_of(t, ra):
        return (chip_counts(ra),) if t == 2 else ()

    def half(t, h):
        n = 2 * STREAM_ROWS[t]
        return pl.ds(h * n, n)

    def relay2(t, h):
        return copy(t, 12 + h, S[t].at[0, 2, half(t, h)], R2[t].at[half(t, h)], 1, 1 if h else 3)

    def own2(t, h):
        if h:
            return copy(t, 14 + h, S[t].at[0, 3, half(t, h)], EM[t].at[half(t, h)], 1, 3)
        return copy(t, 14 + h, S[t].at[0, 1, half(t, h)], EP[t].at[half(t, h)], 1, 1)

    def comb2(t, h):
        if h:
            return copy(t, 16 + h, S[t].at[0, 1, half(t, h)], EP[t].at[half(t, h)], 1, 1)
        return copy(t, 16 + h, S[t].at[0, 3, half(t, h)], EM[t].at[half(t, h)], 1, 3)

    def last3(t, rc):
        n = STREAM_ROWS[t]
        return copy(t, 17 + rc, S[t].at[0, 0, pl.ds(rc * n, n)], D3[t].at[rc - 1], 2, rc)

    done = set()
    held = []
    sent = set()
    def column(rb):
        return [(d, rb) for d in range(4)]

    sends = ([(0, far1, rb, rb, 2, [(rb, 2)]) for rb in (2, 1, 3, 0)]
             + [(1, far1, rb, rb, 2, [(2, rb)]) for rb in (2, 1, 3, 0)]
             + [(2, far1, rb, rb, 2, column(rb)) for rb in (2, 1, 3, 0)]
             + [(0, own1, 4 + rb, rb, ra, [(rb, ra)]) for rb, ra in ((1, 1), (2, 3), (0, 1), (3, 3))]
             + [(1, own1, 4 + rb, rb, ra, [(ra, rb)]) for rb, ra in ((1, 1), (2, 3), (0, 1), (3, 3))]
             + [(2, own1, 4 + rb, rb, ra, column(rb)) for rb, ra in ((1, 1), (2, 3), (0, 1), (3, 3))]
             + [(t, comb1, 8 + rb, rb, 1 if rb >= 2 else 3, column(rb)) for t, rb in DIRECT])
    for pos in range(PIECES):
        if pos == 0 or batch_of(pos) != batch_of(pos - 1):
            batch = [p for p in range(PIECES) if batch_of(p) == batch_of(pos)]
            wait_bytes(xp.at[pl.ds(pos, len(batch))], sem_pr.at[batch_of(pos)])
        weigh(xp, wed_p, 8, pos)
        at = window(pos, core)[1]

        def classes(dy, carry):
            for j in range(2):
                class_sum(pos, at, dy, j)
            return carry

        lax.fori_loop(0, 4, classes, 0, unroll=True)
        done.add(ORDER[pos])
        for i, (t, make, place, rb, ra, needs) in enumerate(sends):
            if i not in sent and done.issuperset(needs):
                sent.add(i)
                encode(QS[t].at[place], S[t][ra, rb], *counts_of(t, ra))
                if make is own1 and pos < HOLD:
                    held.append((t, rb))
                else:
                    make(t, rb).start()
        if pos == HOLD:
            for t, rb in held:
                own1(t, rb).start()

    for t, rb in ((0, 2), (1, 2), (0, 1), (1, 1), (0, 3), (2, 2), (1, 3), (0, 0), (1, 0), (2, 1)):
        far1(t, rb).wait_recv()
        ra = 1 if rb >= 2 else 3
        v, c = decode(Q1[t].at[rb], 4 * STREAM_ROWS[t])
        encode(QS[t].at[8 + rb], S[t][ra, rb] + v, *[n + c for n in counts_of(t, ra)])
        comb1(t, rb).start()
    kept = [None] * 3
    waited = set()

    def wait_ring(t, rb):
        if (t, rb) not in waited:
            waited.add((t, rb))
            wait_bytes(QD[t].at[rb, pl.ds(0, arrivals(t, rb))], sem_rd.at[t, rb])

    wait_ring(0, 2)
    wait_ring(1, 2)
    counts = None
    for t, rb in ((0, 2), (1, 2), (2, 3), (0, 1), (1, 1), (2, 2), (2, 1), (0, 3), (1, 3), (0, 0), (2, 0), (1, 0)):
        wait_ring(t, rb)
        r = STREAM_ROWS[t]
        total = S[t][0, rb]
        seen = chip_counts(0) if t == 2 else None
        for side in range(arrivals(t, rb)):
            v, c = decode(QD[t].at[rb, side], 4 * r)
            total = total + v
            if t == 2:
                seen = seen + c
        if t == 2 and counts is None:
            counts = seen
        more = (counts,) if t == 2 else ()
        for rc in (2, 1, 3, 0):
            part = total[rc * r:(rc + 1) * r]
            if rb or rc:
                encode(QT[t].at[rb * 4 + rc - 1], part, *more)
                plane(t, rb, rc).start()
            else:
                kept[t] = part
    final = []
    for t in (0, 1, 2):
        wait_bytes(QF[t], sem_rf.at[t])
        total = kept[t]
        for m in range(15):
            v, c = decode(QF[t].at[m], STREAM_ROWS[t])
            total = total + v
            if t == 2:
                counts = counts + c
        final.append(total)
    tail, heads = final[2], final[:2]

    counts_lane = lax.broadcasted_iota(jnp.int32, (1, 128), 1)
    even = lax.rem(lax.broadcasted_iota(jnp.int32, (ROWS, 128), 0), 2) == 0
    own_at = window(PIECES - 1, core)[1]
    totals = []
    for j in range(2):
        row = counts[j:j + 1]
        total = jnp.zeros((ROWS, 128), F32)
        for w in range(WEDGES):
            n = jnp.sum(jnp.where(counts_lane == w, row, 0.0), axis=1, keepdims=True)
            a = wexp[PIECES - 1, w, pl.ds(own_at, ROWS), :]
            total = total + n * (a * a)
        totals.append(total)
        summed = jnp.concatenate([heads[j], tail[j * TAIL:(j + 1) * TAIL]], axis=0)
        avg = summed / (total + 1.0)
        avg_ref[j] = avg[0:2 * NB].reshape(NB, 2, 128)
    tot_ref[...] = jnp.where(even, totals[0], totals[1])[0:2 * NB].reshape(NB, 2, 128)
    for t in range(3):
        wait_bytes(QS[t], sem_s1.at[t])
        wait_bytes(QT[t], sem_s2.at[t])
    wait_bytes(xp, sem_ps)
    lab_copy.wait_send()
    wed_copy.wait_send()


def put_out(avg_ref, tot_ref, avg_out, tot_out, sems):
    one = pltpu.make_async_copy(avg_ref, avg_out, sems.at[0])
    two = pltpu.make_async_copy(tot_ref, tot_out, sems.at[1])
    one.start()
    two.start()
    one.wait()
    two.wait()


def per_device(particles, labels, wedge_index, wedge_table):
    x = particles.reshape(PDEV, 2, 32 * NB, 128).transpose(0, 2, 1, 3)
    x = x.reshape(PDEV, 64 * NB, 128)
    lab = labels.reshape(PDEV)
    hbm = pl.BlockSpec(memory_space=pltpu.HBM)
    vmem = pl.BlockSpec(memory_space=pltpu.VMEM)
    dma = pltpu.SemaphoreType.DMA
    V = pltpu.VMEM

    def per_stream(*lead):
        return [V((*lead, 4 * r, 128), F32) for r in STREAM_ROWS]

    def coded(*lead):
        return [V((*lead, 4 * r + extra, 128), jnp.int16)
                for r, extra in zip(STREAM_ROWS, (8, 8, 16))]

    shapes = (jax.ShapeDtypeStruct((2, NB, 2, 128), F32),
              jax.ShapeDtypeStruct((NB, 2, 128), F32))
    avg, tot = pl.pallas_call(
        kernel,
        out_shape=shapes,
        in_specs=[hbm] * 4,
        out_specs=(vmem, vmem),
        scratch_shapes=[
            V((PIECES, PDEV, WINDOW, 128), BF16),
            V((PIECES, PDEV, WINDOW, 128), BF16),
            V((PIECES * 16 + 1, WROWS, 128), F32),
            V((PIECES, WEDGES, NB * 128), F32),
            V((PIECES, WEDGES, WROWS, 128), F32),
            *[pltpu.SMEM((PDEV,), jnp.int32)] * 4,
            pltpu.SMEM((32,), jnp.int32),
            pltpu.SMEM((32,), jnp.int32),
            *per_stream(4, 4),
            *coded(12), *coded(4), *coded(4, 3),
            *[V((15, HEAD + 8, 128), jnp.int16)] * 6,
            dma((4,)), dma((4,)), dma((2,)), dma(()), dma((9,)), dma((2,)), dma((2,)),
            dma((3,)), dma((3,)), dma((3, 4)), dma((3, 4)), dma((3,)),
        ],
        compiler_params=pltpu.CompilerParams(
            collective_id=0, has_side_effects=True, vmem_limit_bytes=44 * 1024 * 1024),
        name="class_sums",
    )(*[pltpu.with_memory_space_constraint(a, pltpu.HBM) for a in (lab, wedge_index, x, wedge_table)])
    avg, tot = pl.pallas_call(
        put_out,
        out_shape=shapes,
        in_specs=[vmem] * 2,
        out_specs=(hbm, hbm),
        scratch_shapes=[dma((2,))],
        compiler_params=pltpu.CompilerParams(vmem_limit_bytes=1024 * 1024),
        name="put_out",
    )(avg, tot)
    avg = avg.transpose(0, 2, 1, 3).reshape(2, 2, NB * 128)
    tot = tot.transpose(1, 0, 2).reshape(2, NB * 128)
    return avg, tot


def solution(mesh):
    return jax.shard_map(
        per_device,
        mesh=mesh,
        in_specs=(P(("cls", "dom"), None, None), P(("cls", "dom"), None), P(("cls", "dom")), P()),
        out_specs=(P("cls", None, "dom"), P("cls", "dom")),
        check_vma=False,
    )
```

```python
import jax
import jax.numpy as jnp
from jax import lax
from jax.experimental import pallas as pl
from jax.experimental.pallas import tpu as pltpu
from jax.sharding import PartitionSpec as P

F32 = jnp.float32
BF16 = jnp.bfloat16
MESH = pl.DeviceIdType.MESH
NB = 27
ROWS = 56
WEDGES = 12
PDEV = 8
PIECES = 16
HEAD = 40
TAIL = ROWS - HEAD
STREAM_ROWS = (HEAD, HEAD, 2 * TAIL)
WINDOW = 64
WROWS = 72
EMPTY = 10000
TOP = 32700.0
STEPS = 64.0
LN2 = 0.6931471805599453
AXES = (("x", "z", "y"), ("z", "x", "y"), ("y", "x", "z"))
ORDER = ((2, 2), (1, 2), (2, 1), (3, 2), (2, 3), (0, 2), (2, 0), (1, 1),
         (0, 1), (3, 1), (3, 3), (1, 3), (0, 3), (1, 0), (3, 0), (0, 0))
BATCH = (0, 1, 2, 3, 4, 5, 5, 6, 6, 6, 7, 7, 7, 8, 8, 8)
HOLD = 7
DIRECT = ((2, 3), (2, 0))


def kernel(lab_hbm, wed_hbm, x_hbm, table_hbm, avg_ref, tot_ref,
           xo, xp, prod, tb, wexp, lab, wed, lab_p, wed_p, slot_p, slot_w,
           s0, s1, s2, qs_0, qs_1, qs_2, q1_0, q1_1, q1_2, qd_0, qd_1, qd_2,
           qt_0, qt_1, qt_2, qf_0, qf_1, qf_2,
           sem_x, sem_t, sem_l, sem_ps, sem_pr, sem_ls, sem_lr,
           sem_s1, sem_s2, sem_r1, sem_rd, sem_rf):
    S = (s0, s1, s2)
    QS = (qs_0, qs_1, qs_2)
    Q1 = (q1_0, q1_1, q1_2)
    QD = (qd_0, qd_1, qd_2)
    QT = (qt_0, qt_1, qt_2)
    QF = (qf_0, qf_1, qf_2)
    y = lax.axis_index("cls")
    dom = lax.axis_index("dom")
    core = lax.rem(dom, 2)
    xc = lax.rem(dom // 2, 4)
    zc = dom // 8

    def device(dz=0, dx=0, dy=0, flip=False):
        c = 1 - core if flip else core
        zz, xx, yy = lax.rem(zc + dz, 4), lax.rem(xc + dx, 4), lax.rem(y + dy, 4)
        return (yy, (zz * 4 + xx) * 2 + c)

    def along(axis, step):
        return device(**{"d" + axis: step})

    partner = device(flip=True)
    barrier = pltpu.get_barrier_semaphore()
    peers = [partner] + [along(a, s) for a in "xyz" for s in (1, 3, 2)]
    for peer in peers:
        pl.semaphore_signal(barrier, inc=1, device_id=peer, device_id_type=MESH)

    def shard_of(pos, c):
        dz, dx = ORDER[pos]
        return (lax.rem(zc + dz, 4) * 4 + lax.rem(xc + dx, 4)) * 2 + c

    def window(pos, c):
        row = shard_of(pos, c) * (2 * NB)
        start = jnp.minimum(row // 8, (64 * NB - WINDOW) // 8) * 8
        return pl.multiple_of(start, 8), row - start

    def own_copy(pos):
        start, _ = window(pos, core)
        return pltpu.make_async_copy(
            x_hbm.at[:, pl.ds(start, WINDOW)], xo.at[pos], sem_x.at[pos // 4])

    def table_copy(pos):
        start = pl.multiple_of(shard_of(pos, core) * (NB * 128), 128)
        return pltpu.make_async_copy(
            table_hbm.at[:, pl.ds(start, NB * 128)], tb.at[pos], sem_t.at[pos // 4])

    def batch_of(pos):
        return BATCH[pos]

    def partner_copy(pos):
        start, _ = window(pos, 1 - core)
        return pltpu.make_async_remote_copy(
            src_ref=x_hbm.at[:, pl.ds(start, WINDOW)], dst_ref=xp.at[pos],
            send_sem=sem_ps, recv_sem=sem_pr.at[batch_of(pos)],
            device_id=partner, device_id_type=MESH)

    def wait_bytes(ref, sem):
        pltpu.make_async_copy(ref, ref, sem).wait()

    lab_local = pltpu.make_async_copy(lab_hbm, lab, sem_l.at[0])
    wed_local = pltpu.make_async_copy(wed_hbm, wed, sem_l.at[1])
    lab_local.start()
    wed_local.start()
    for pos in range(PIECES):
        table_copy(pos).start()
        own_copy(pos).start()
    pl.semaphore_wait(barrier, len(peers))

    lab_copy = pltpu.make_async_remote_copy(
        src_ref=lab_hbm, dst_ref=lab_p, send_sem=sem_ls.at[0], recv_sem=sem_lr.at[0],
        device_id=partner, device_id_type=MESH)
    wed_copy = pltpu.make_async_remote_copy(
        src_ref=wed_hbm, dst_ref=wed_p, send_sem=sem_ls.at[1], recv_sem=sem_lr.at[1],
        device_id=partner, device_id_type=MESH)
    lab_copy.start()
    wed_copy.start()
    for pos in range(PIECES):
        partner_copy(pos).start()

    def slots(lab_ref, wed_ref, base):
        labels = [lab_ref[p] for p in range(PDEV)]

        def one_class(k, carry):
            p1, p2 = jnp.int32(EMPTY), jnp.int32(-1)
            for p in range(PDEV):
                hit = labels[p] == k
                p1 = jnp.where(hit, jnp.minimum(p1, p), p1)
                p2 = jnp.where(hit, p, p2)
            one, two = p1 < PDEV, p2 > p1
            w1 = wed_ref[jnp.minimum(p1, PDEV - 1)]
            w2 = wed_ref[jnp.maximum(p2, 0)]
            slot_p[k * 4 + base] = jnp.where(one, base * 4 + p1, EMPTY)
            slot_w[k * 4 + base] = jnp.where(one, w1, WEDGES)
            slot_p[k * 4 + base + 1] = jnp.where(two, base * 4 + p2, EMPTY)
            slot_w[k * 4 + base + 1] = jnp.where(two, w2, WEDGES)
            return carry

        lax.fori_loop(0, 8, one_class, 0, unroll=True)

    lab_local.wait()
    wed_local.wait()
    slots(lab, wed, 0)

    def expand(pos):
        rows = wexp.at[pos].reshape(WEDGES * WROWS, 128)
        at = window(pos, core)[1]
        for b in range(NB):
            for lo, n in ((0, 8), (8, WEDGES - 8)):
                v = tb[pos, pl.ds(lo, n), pl.ds(b * 128, 128)]
                for c in range(2):
                    rows[pl.ds(at + lo * WROWS + 2 * b + c, n, stride=WROWS), :] = v

    def weigh(src, wedges, base, pos):
        for p in range(PDEV):
            prod[pos * 16 + base + p, pl.ds(0, WINDOW), :] = (
                src[pos, p].astype(F32) * wexp[pos, wedges[p], pl.ds(0, WINDOW), :])

    prod[PIECES * 16] = jnp.zeros((WROWS, 128), F32)

    for pos in range(PIECES):
        if pos % 4 == 0:
            wait_bytes(tb.at[pl.ds(pos, 4)], sem_t.at[pos // 4])
            wait_bytes(xo.at[pl.ds(pos, 4)], sem_x.at[pos // 4])
        expand(pos)
        weigh(xo, wed, 0, pos)

    lab_copy.wait_recv()
    wed_copy.wait_recv()
    slots(lab_p, wed_p, 2)

    sub = lax.broadcasted_iota(jnp.int32, (TAIL, 128), 0)
    sub8 = lax.broadcasted_iota(jnp.int32, (8, 128), 0)
    lane8 = lax.broadcasted_iota(jnp.int32, (8, 128), 1)

    def chip_counts(dy):
        total = jnp.zeros((8, 128), F32)
        for j in range(2):
            k = lax.rem(y + dy, 4) * 2 + j
            for s in range(4):
                total = total + ((lane8 == slot_w[k * 4 + s]) & (sub8 == j)).astype(F32)
        return total

    def encode(dst, v, *more):
        n = v.shape[0]
        v = v.reshape(n // 8, 8, 128)
        top = jnp.maximum(jnp.max(jnp.abs(v), axis=0), 1e-30)
        code = jnp.ceil(jnp.log(top) * (STEPS / LN2))
        q = jnp.round(v * (jnp.exp(code * (-LN2 / STEPS)) * TOP)[None])
        rows = jnp.concatenate([q.reshape(n, 128), code, *more], axis=0)
        dst[...] = rows.astype(jnp.int32).astype(jnp.int16)

    def decode(src, n):
        rows = src[...].astype(jnp.int32).astype(F32)
        scale = jnp.exp(rows[n:n + 8] * (LN2 / STEPS)) * (1.0 / TOP)
        return (rows[0:n].reshape(n // 8, 8, 128) * scale[None]).reshape(n, 128), rows[n + 8:]

    def class_sum(piece, at, dy, j):
        dz, dx = ORDER[piece]
        k = lax.rem(y + dy, 4) * 2 + j
        total = None
        for s in range(4):
            place = jnp.minimum(slot_p[k * 4 + s] + piece * 16, PIECES * 16)
            v = prod[place, pl.ds(at, ROWS), :]
            total = v if total is None else total + v
        tail = jnp.where(sub < TAIL - 2, total[HEAD:ROWS], 0.0)
        if j == 0:
            S[0][dx, dz, pl.ds(dy * HEAD, HEAD), :] = total[0:HEAD]
        else:
            S[1][dz, dx, pl.ds(dy * HEAD, HEAD), :] = total[0:HEAD]
        S[2][dy, dx, pl.ds(dz * 2 * TAIL + j * TAIL, TAIL), :] = tail

    def ring(t, src, dst, recv, step):
        return pltpu.make_async_remote_copy(
            src_ref=src, dst_ref=dst, send_sem=sem_s1.at[t], recv_sem=recv,
            device_id=along(AXES[t][0], step), device_id_type=MESH)

    def far1(t, rb):
        if (t, rb) in DIRECT:
            return ring(t, QS[t].at[rb], QD[t].at[rb, 2], sem_rd.at[t, rb], 2)
        return ring(t, QS[t].at[rb], Q1[t].at[rb], sem_r1.at[t, rb], 1 if rb >= 2 else 3)

    def own1(t, rb):
        side = 1 if rb >= 2 else 0
        return ring(t, QS[t].at[4 + rb], QD[t].at[rb, side], sem_rd.at[t, rb], 3 if side else 1)

    def comb1(t, rb):
        side = 0 if rb >= 2 else 1
        return ring(t, QS[t].at[8 + rb], QD[t].at[rb, side], sem_rd.at[t, rb], 3 if side else 1)

    def arrivals(t, rb):
        return 3 if (t, rb) in DIRECT else 2

    def plane(t, rb, rc):
        m = rb * 4 + rc - 1
        target = device(**{"d" + AXES[t][1]: rb, "d" + AXES[t][2]: rc})
        return pltpu.make_async_remote_copy(
            src_ref=QT[t].at[m], dst_ref=QF[t].at[m],
            send_sem=sem_s2.at[t], recv_sem=sem_rf.at[t],
            device_id=target, device_id_type=MESH)

    def counts_of(t, ra):
        return (chip_counts(ra),) if t == 2 else ()

    def half(t, h):
        n = 2 * STREAM_ROWS[t]
        return pl.ds(h * n, n)

    def relay2(t, h):
        return copy(t, 12 + h, S[t].at[0, 2, half(t, h)], R2[t].at[half(t, h)], 1, 1 if h else 3)

    def own2(t, h):
        if h:
            return copy(t, 14 + h, S[t].at[0, 3, half(t, h)], EM[t].at[half(t, h)], 1, 3)
        return copy(t, 14 + h, S[t].at[0, 1, half(t, h)], EP[t].at[half(t, h)], 1, 1)

    def comb2(t, h):
        if h:
            return copy(t, 16 + h, S[t].at[0, 1, half(t, h)], EP[t].at[half(t, h)], 1, 1)
        return copy(t, 16 + h, S[t].at[0, 3, half(t, h)], EM[t].at[half(t, h)], 1, 3)

    def last3(t, rc):
        n = STREAM_ROWS[t]
        return copy(t, 17 + rc, S[t].at[0, 0, pl.ds(rc * n, n)], D3[t].at[rc - 1], 2, rc)

    done = set()
    held = []
    sent = set()
    def column(rb):
        return [(d, rb) for d in range(4)]

    sends = ([(0, far1, rb, rb, 2, [(rb, 2)]) for rb in (2, 1, 3, 0)]
             + [(1, far1, rb, rb, 2, [(2, rb)]) for rb in (2, 1, 3, 0)]
             + [(2, far1, rb, rb, 2, column(rb)) for rb in (2, 1, 3, 0)]
             + [(0, own1, 4 + rb, rb, ra, [(rb, ra)]) for rb, ra in ((1, 1), (2, 3), (0, 1), (3, 3))]
             + [(1, own1, 4 + rb, rb, ra, [(ra, rb)]) for rb, ra in ((1, 1), (2, 3), (0, 1), (3, 3))]
             + [(2, own1, 4 + rb, rb, ra, column(rb)) for rb, ra in ((1, 1), (2, 3), (0, 1), (3, 3))]
             + [(t, comb1, 8 + rb, rb, 1 if rb >= 2 else 3, column(rb)) for t, rb in DIRECT])
    for pos in range(PIECES):
        if pos == 0 or batch_of(pos) != batch_of(pos - 1):
            batch = [p for p in range(PIECES) if batch_of(p) == batch_of(pos)]
            wait_bytes(xp.at[pl.ds(pos, len(batch))], sem_pr.at[batch_of(pos)])
        weigh(xp, wed_p, 8, pos)
        at = window(pos, core)[1]

        def classes(dy, carry):
            for j in range(2):
                class_sum(pos, at, dy, j)
            return carry

        lax.fori_loop(0, 4, classes, 0, unroll=True)
        done.add(ORDER[pos])
        for i, (t, make, place, rb, ra, needs) in enumerate(sends):
            if i not in sent and done.issuperset(needs):
                sent.add(i)
                encode(QS[t].at[place], S[t][ra, rb], *counts_of(t, ra))
                if make is own1 and pos < HOLD:
                    held.append((t, rb))
                else:
                    make(t, rb).start()
        if pos == HOLD:
            for t, rb in held:
                own1(t, rb).start()

    for t, rb in ((0, 2), (1, 2), (0, 1), (1, 1), (0, 3), (2, 2), (1, 3), (0, 0), (1, 0), (2, 1)):
        far1(t, rb).wait_recv()
        ra = 1 if rb >= 2 else 3
        v, c = decode(Q1[t].at[rb], 4 * STREAM_ROWS[t])
        encode(QS[t].at[8 + rb], S[t][ra, rb] + v, *[n + c for n in counts_of(t, ra)])
        comb1(t, rb).start()
    kept = [None] * 3
    waited = set()

    def wait_ring(t, rb):
        if (t, rb) not in waited:
            waited.add((t, rb))
            wait_bytes(QD[t].at[rb, pl.ds(0, arrivals(t, rb))], sem_rd.at[t, rb])

    wait_ring(0, 2)
    wait_ring(1, 2)
    counts = None
    for t, rb in ((0, 2), (1, 2), (2, 3), (0, 1), (1, 1), (2, 2), (2, 1), (0, 3), (1, 3), (0, 0), (2, 0), (1, 0)):
        wait_ring(t, rb)
        r = STREAM_ROWS[t]
        total = S[t][0, rb]
        seen = chip_counts(0) if t == 2 else None
        for side in range(arrivals(t, rb)):
            v, c = decode(QD[t].at[rb, side], 4 * r)
            total = total + v
            if t == 2:
                seen = seen + c
        if t == 2 and counts is None:
            counts = seen
        more = (counts,) if t == 2 else ()
        for rc in (2, 1, 3, 0):
            part = total[rc * r:(rc + 1) * r]
            if rb or rc:
                encode(QT[t].at[rb * 4 + rc - 1], part, *more)
                plane(t, rb, rc).start()
            else:
                kept[t] = part
    final = []
    for t in (0, 1, 2):
        wait_bytes(QF[t], sem_rf.at[t])
        total = kept[t]
        for m in range(15):
            v, c = decode(QF[t].at[m], STREAM_ROWS[t])
            total = total + v
            if t == 2:
                counts = counts + c
        final.append(total)
    tail, heads = final[2], final[:2]

    counts_lane = lax.broadcasted_iota(jnp.int32, (1, 128), 1)
    even = lax.rem(lax.broadcasted_iota(jnp.int32, (ROWS, 128), 0), 2) == 0
    own_at = window(PIECES - 1, core)[1]
    totals = []
    for j in range(2):
        row = counts[j:j + 1]
        total = jnp.zeros((ROWS, 128), F32)
        for w in range(WEDGES):
            n = jnp.sum(jnp.where(counts_lane == w, row, 0.0), axis=1, keepdims=True)
            a = wexp[PIECES - 1, w, pl.ds(own_at, ROWS), :]
            total = total + n * (a * a)
        totals.append(total)
        summed = jnp.concatenate([heads[j], tail[j * TAIL:(j + 1) * TAIL]], axis=0)
        avg = summed / (total + 1.0)
        avg_ref[j] = avg[0:2 * NB].reshape(NB, 2, 128)
    tot_ref[...] = jnp.where(even, totals[0], totals[1])[0:2 * NB].reshape(NB, 2, 128)
    for t in range(3):
        wait_bytes(QS[t], sem_s1.at[t])
        wait_bytes(QT[t], sem_s2.at[t])
    wait_bytes(xp, sem_ps)
    lab_copy.wait_send()
    wed_copy.wait_send()


def put_out(avg_ref, tot_ref, avg_out, tot_out, sems):
    one = pltpu.make_async_copy(avg_ref, avg_out, sems.at[0])
    two = pltpu.make_async_copy(tot_ref, tot_out, sems.at[1])
    one.start()
    two.start()
    one.wait()
    two.wait()


def per_device(particles, labels, wedge_index, wedge_table):
    x = particles.reshape(PDEV, 2, 32 * NB, 128).transpose(0, 2, 1, 3)
    x = x.reshape(PDEV, 64 * NB, 128)
    lab = labels.reshape(PDEV)
    hbm = pl.BlockSpec(memory_space=pltpu.HBM)
    vmem = pl.BlockSpec(memory_space=pltpu.VMEM)
    dma = pltpu.SemaphoreType.DMA
    V = pltpu.VMEM

    def per_stream(*lead):
        return [V((*lead, 4 * r, 128), F32) for r in STREAM_ROWS]

    def coded(*lead):
        return [V((*lead, 4 * r + extra, 128), jnp.int16)
                for r, extra in zip(STREAM_ROWS, (8, 8, 16))]

    shapes = (jax.ShapeDtypeStruct((2, NB, 2, 128), F32),
              jax.ShapeDtypeStruct((NB, 2, 128), F32))
    avg, tot = pl.pallas_call(
        kernel,
        out_shape=shapes,
        in_specs=[hbm] * 4,
        out_specs=(vmem, vmem),
        scratch_shapes=[
            V((PIECES, PDEV, WINDOW, 128), BF16),
            V((PIECES, PDEV, WINDOW, 128), BF16),
            V((PIECES * 16 + 1, WROWS, 128), F32),
            V((PIECES, WEDGES, NB * 128), F32),
            V((PIECES, WEDGES, WROWS, 128), F32),
            *[pltpu.SMEM((PDEV,), jnp.int32)] * 4,
            pltpu.SMEM((32,), jnp.int32),
            pltpu.SMEM((32,), jnp.int32),
            *per_stream(4, 4),
            *coded(12), *coded(4), *coded(4, 3),
            *[V((15, HEAD + 8, 128), jnp.int16)] * 6,
            dma((4,)), dma((4,)), dma((2,)), dma(()), dma((9,)), dma((2,)), dma((2,)),
            dma((3,)), dma((3,)), dma((3, 4)), dma((3, 4)), dma((3,)),
        ],
        compiler_params=pltpu.CompilerParams(
            collective_id=0, has_side_effects=True, vmem_limit_bytes=44 * 1024 * 1024),
        name="class_sums",
    )(*[pltpu.with_memory_space_constraint(a, pltpu.HBM) for a in (lab, wedge_index, x, wedge_table)])
    avg, tot = pl.pallas_call(
        put_out,
        out_shape=shapes,
        in_specs=[vmem] * 2,
        out_specs=(hbm, hbm),
        scratch_shapes=[dma((2,))],
        compiler_params=pltpu.CompilerParams(vmem_limit_bytes=1024 * 1024),
        name="put_out",
    )(avg, tot)
    avg = avg.transpose(0, 2, 1, 3).reshape(2, 2, NB * 128)
    tot = tot.transpose(1, 0, 2).reshape(2, NB * 128)
    return avg, tot


def solution(mesh):
    return jax.shard_map(
        per_device,
        mesh=mesh,
        in_specs=(P(("cls", "dom"), None, None), P(("cls", "dom"), None), P(("cls", "dom")), P()),
        out_specs=(P("cls", None, "dom"), P("cls", "dom")),
        check_vma=False,
    )
```

```python
import jax
import jax.numpy as jnp
from jax import lax
from jax.experimental import pallas as pl
from jax.experimental.pallas import tpu as pltpu
from jax.sharding import PartitionSpec as P

F32 = jnp.float32
BF16 = jnp.bfloat16
MESH = pl.DeviceIdType.MESH
NB = 27
ROWS = 56
WEDGES = 12
PDEV = 8
PIECES = 16
HEAD = 40
TAIL = ROWS - HEAD
STREAM_ROWS = (HEAD, HEAD, 2 * TAIL)
WINDOW = 64
WROWS = 72
EMPTY = 10000
TOP = 32700.0
STEPS = 64.0
LN2 = 0.6931471805599453
AXES = (("x", "z", "y"), ("z", "x", "y"), ("y", "x", "z"))
ORDER = ((2, 2), (1, 2), (2, 1), (3, 2), (2, 3), (0, 2), (2, 0), (1, 1),
         (0, 1), (3, 1), (3, 3), (1, 3), (0, 3), (1, 0), (3, 0), (0, 0))
BATCH = (0, 1, 2, 3, 4, 5, 5, 6, 6, 6, 7, 7, 7, 8, 8, 8)
HOLD = 7
DIRECT = ((2, 3), (2, 0))


def kernel(lab_hbm, wed_hbm, x_hbm, table_hbm, avg_ref, tot_ref,
           xo, xp, prod, tb, wexp, lab, wed, lab_p, wed_p, slot_p, slot_w,
           s0, s1, s2, qs_0, qs_1, qs_2, q1_0, q1_1, q1_2, qd_0, qd_1, qd_2,
           qt_0, qt_1, qt_2, qf_0, qf_1, qf_2,
           sem_x, sem_t, sem_l, sem_ps, sem_pr, sem_ls, sem_lr,
           sem_s1, sem_s2, sem_r1, sem_rd, sem_rf):
    S = (s0, s1, s2)
    QS = (qs_0, qs_1, qs_2)
    Q1 = (q1_0, q1_1, q1_2)
    QD = (qd_0, qd_1, qd_2)
    QT = (qt_0, qt_1, qt_2)
    QF = (qf_0, qf_1, qf_2)
    y = lax.axis_index("cls")
    dom = lax.axis_index("dom")
    core = lax.rem(dom, 2)
    xc = lax.rem(dom // 2, 4)
    zc = dom // 8

    def device(dz=0, dx=0, dy=0, flip=False):
        c = 1 - core if flip else core
        zz, xx, yy = lax.rem(zc + dz, 4), lax.rem(xc + dx, 4), lax.rem(y + dy, 4)
        return (yy, (zz * 4 + xx) * 2 + c)

    def along(axis, step):
        return device(**{"d" + axis: step})

    partner = device(flip=True)
    barrier = pltpu.get_barrier_semaphore()
    peers = [partner] + [along(a, s) for a in "xyz" for s in (1, 3, 2)]
    for peer in peers:
        pl.semaphore_signal(barrier, inc=1, device_id=peer, device_id_type=MESH)

    def shard_of(pos, c):
        dz, dx = ORDER[pos]
        return (lax.rem(zc + dz, 4) * 4 + lax.rem(xc + dx, 4)) * 2 + c

    def window(pos, c):
        row = shard_of(pos, c) * (2 * NB)
        start = jnp.minimum(row // 8, (64 * NB - WINDOW) // 8) * 8
        return pl.multiple_of(start, 8), row - start

    def own_copy(pos):
        start, _ = window(pos, core)
        return pltpu.make_async_copy(
            x_hbm.at[:, pl.ds(start, WINDOW)], xo.at[pos], sem_x.at[pos // 4])

    def table_copy(pos):
        start = pl.multiple_of(shard_of(pos, core) * (NB * 128), 128)
        return pltpu.make_async_copy(
            table_hbm.at[:, pl.ds(start, NB * 128)], tb.at[pos], sem_t.at[pos // 4])

    def batch_of(pos):
        return BATCH[pos]

    def partner_copy(pos):
        start, _ = window(pos, 1 - core)
        return pltpu.make_async_remote_copy(
            src_ref=x_hbm.at[:, pl.ds(start, WINDOW)], dst_ref=xp.at[pos],
            send_sem=sem_ps, recv_sem=sem_pr.at[batch_of(pos)],
            device_id=partner, device_id_type=MESH)

    def wait_bytes(ref, sem):
        pltpu.make_async_copy(ref, ref, sem).wait()

    lab_local = pltpu.make_async_copy(lab_hbm, lab, sem_l.at[0])
    wed_local = pltpu.make_async_copy(wed_hbm, wed, sem_l.at[1])
    lab_local.start()
    wed_local.start()
    for pos in range(PIECES):
        table_copy(pos).start()
        own_copy(pos).start()
    pl.semaphore_wait(barrier, len(peers))

    lab_copy = pltpu.make_async_remote_copy(
        src_ref=lab_hbm, dst_ref=lab_p, send_sem=sem_ls.at[0], recv_sem=sem_lr.at[0],
        device_id=partner, device_id_type=MESH)
    wed_copy = pltpu.make_async_remote_copy(
        src_ref=wed_hbm, dst_ref=wed_p, send_sem=sem_ls.at[1], recv_sem=sem_lr.at[1],
        device_id=partner, device_id_type=MESH)
    for pos in range(PIECES):
        if pos == 3:
            lab_copy.start()
            wed_copy.start()
        partner_copy(pos).start()

    def slots(lab_ref, wed_ref, base):
        labels = [lab_ref[p] for p in range(PDEV)]
        wedges = [wed_ref[p] for p in range(PDEV)]

        def one_class(k, carry):
            p1, w1, p2, w2 = EMPTY, WEDGES, EMPTY, WEDGES
            seen = jnp.int32(0)
            for p in range(PDEV):
                hit = labels[p] == k
                first = hit & (seen == 0)
                second = hit & (seen > 0)
                p1 = jnp.where(first, base * 4 + p, p1)
                w1 = jnp.where(first, wedges[p], w1)
                p2 = jnp.where(second, base * 4 + p, p2)
                w2 = jnp.where(second, wedges[p], w2)
                seen = seen + hit.astype(jnp.int32)
            slot_p[k * 4 + base] = p1
            slot_w[k * 4 + base] = w1
            slot_p[k * 4 + base + 1] = p2
            slot_w[k * 4 + base + 1] = w2
            return carry

        lax.fori_loop(0, 8, one_class, 0)

    lab_local.wait()
    wed_local.wait()
    slots(lab, wed, 0)

    def expand(pos):
        rows = wexp.at[pos].reshape(WEDGES * WROWS, 128)
        at = window(pos, core)[1]
        for b in range(NB):
            for lo, n in ((0, 8), (8, WEDGES - 8)):
                v = tb[pos, pl.ds(lo, n), pl.ds(b * 128, 128)]
                for c in range(2):
                    rows[pl.ds(at + lo * WROWS + 2 * b + c, n, stride=WROWS), :] = v

    def weigh(src, wedges, base, pos):
        for p in range(PDEV):
            prod[pos * 16 + base + p, pl.ds(0, WINDOW), :] = (
                src[pos, p].astype(F32) * wexp[pos, wedges[p], pl.ds(0, WINDOW), :])

    prod[PIECES * 16] = jnp.zeros((WROWS, 128), F32)

    for pos in range(PIECES):
        if pos % 4 == 0:
            wait_bytes(tb.at[pl.ds(pos, 4)], sem_t.at[pos // 4])
            wait_bytes(xo.at[pl.ds(pos, 4)], sem_x.at[pos // 4])
        expand(pos)
        weigh(xo, wed, 0, pos)

    lab_copy.wait_recv()
    wed_copy.wait_recv()
    slots(lab_p, wed_p, 2)

    sub = lax.broadcasted_iota(jnp.int32, (TAIL, 128), 0)
    sub8 = lax.broadcasted_iota(jnp.int32, (8, 128), 0)
    lane8 = lax.broadcasted_iota(jnp.int32, (8, 128), 1)

    def chip_counts(dy):
        total = jnp.zeros((8, 128), F32)
        for j in range(2):
            k = lax.rem(y + dy, 4) * 2 + j
            for s in range(4):
                total = total + ((lane8 == slot_w[k * 4 + s]) & (sub8 == j)).astype(F32)
        return total

    def encode(dst, v, *more):
        n = v.shape[0]
        v = v.reshape(n // 8, 8, 128)
        top = jnp.maximum(jnp.max(jnp.abs(v), axis=0), 1e-30)
        code = jnp.ceil(jnp.log(top) * (STEPS / LN2))
        q = jnp.round(v * (jnp.exp(code * (-LN2 / STEPS)) * TOP)[None])
        rows = jnp.concatenate([q.reshape(n, 128), code, *more], axis=0)
        dst[...] = rows.astype(jnp.int32).astype(jnp.int16)

    def decode(src, n):
        rows = src[...].astype(jnp.int32).astype(F32)
        scale = jnp.exp(rows[n:n + 8] * (LN2 / STEPS)) * (1.0 / TOP)
        return (rows[0:n].reshape(n // 8, 8, 128) * scale[None]).reshape(n, 128), rows[n + 8:]

    def class_sum(piece, at, dy, j):
        dz, dx = ORDER[piece]
        k = lax.rem(y + dy, 4) * 2 + j
        total = None
        for s in range(4):
            place = jnp.minimum(slot_p[k * 4 + s] + piece * 16, PIECES * 16)
            v = prod[place, pl.ds(at, ROWS), :]
            total = v if total is None else total + v
        tail = jnp.where(sub < TAIL - 2, total[HEAD:ROWS], 0.0)
        if j == 0:
            S[0][dx, dz, pl.ds(dy * HEAD, HEAD), :] = total[0:HEAD]
        else:
            S[1][dz, dx, pl.ds(dy * HEAD, HEAD), :] = total[0:HEAD]
        S[2][dy, dx, pl.ds(dz * 2 * TAIL + j * TAIL, TAIL), :] = tail

    def ring(t, src, dst, recv, step):
        return pltpu.make_async_remote_copy(
            src_ref=src, dst_ref=dst, send_sem=sem_s1.at[t], recv_sem=recv,
            device_id=along(AXES[t][0], step), device_id_type=MESH)

    def far1(t, rb):
        if (t, rb) in DIRECT:
            return ring(t, QS[t].at[rb], QD[t].at[rb, 2], sem_rd.at[t, rb], 2)
        return ring(t, QS[t].at[rb], Q1[t].at[rb], sem_r1.at[t, rb], 1 if rb >= 2 else 3)

    def own1(t, rb):
        side = 1 if rb >= 2 else 0
        return ring(t, QS[t].at[4 + rb], QD[t].at[rb, side], sem_rd.at[t, rb], 3 if side else 1)

    def comb1(t, rb):
        side = 0 if rb >= 2 else 1
        return ring(t, QS[t].at[8 + rb], QD[t].at[rb, side], sem_rd.at[t, rb], 3 if side else 1)

    def arrivals(t, rb):
        return 3 if (t, rb) in DIRECT else 2

    def plane(t, rb, rc):
        m = rb * 4 + rc - 1
        target = device(**{"d" + AXES[t][1]: rb, "d" + AXES[t][2]: rc})
        return pltpu.make_async_remote_copy(
            src_ref=QT[t].at[m], dst_ref=QF[t].at[m],
            send_sem=sem_s2.at[t], recv_sem=sem_rf.at[t],
            device_id=target, device_id_type=MESH)

    def counts_of(t, ra):
        return (chip_counts(ra),) if t == 2 else ()

    def half(t, h):
        n = 2 * STREAM_ROWS[t]
        return pl.ds(h * n, n)

    def relay2(t, h):
        return copy(t, 12 + h, S[t].at[0, 2, half(t, h)], R2[t].at[half(t, h)], 1, 1 if h else 3)

    def own2(t, h):
        if h:
            return copy(t, 14 + h, S[t].at[0, 3, half(t, h)], EM[t].at[half(t, h)], 1, 3)
        return copy(t, 14 + h, S[t].at[0, 1, half(t, h)], EP[t].at[half(t, h)], 1, 1)

    def comb2(t, h):
        if h:
            return copy(t, 16 + h, S[t].at[0, 1, half(t, h)], EP[t].at[half(t, h)], 1, 1)
        return copy(t, 16 + h, S[t].at[0, 3, half(t, h)], EM[t].at[half(t, h)], 1, 3)

    def last3(t, rc):
        n = STREAM_ROWS[t]
        return copy(t, 17 + rc, S[t].at[0, 0, pl.ds(rc * n, n)], D3[t].at[rc - 1], 2, rc)

    done = set()
    held = []
    sent = set()
    def column(rb):
        return [(d, rb) for d in range(4)]

    sends = ([(0, far1, rb, rb, 2, [(rb, 2)]) for rb in (2, 1, 3, 0)]
             + [(1, far1, rb, rb, 2, [(2, rb)]) for rb in (2, 1, 3, 0)]
             + [(2, far1, rb, rb, 2, column(rb)) for rb in (2, 1, 3, 0)]
             + [(0, own1, 4 + rb, rb, ra, [(rb, ra)]) for rb, ra in ((1, 1), (2, 3), (0, 1), (3, 3))]
             + [(1, own1, 4 + rb, rb, ra, [(ra, rb)]) for rb, ra in ((1, 1), (2, 3), (0, 1), (3, 3))]
             + [(2, own1, 4 + rb, rb, ra, column(rb)) for rb, ra in ((1, 1), (2, 3), (0, 1), (3, 3))]
             + [(t, comb1, 8 + rb, rb, 1 if rb >= 2 else 3, column(rb)) for t, rb in DIRECT])
    for pos in range(PIECES):
        if pos == 0 or batch_of(pos) != batch_of(pos - 1):
            batch = [p for p in range(PIECES) if batch_of(p) == batch_of(pos)]
            wait_bytes(xp.at[pl.ds(pos, len(batch))], sem_pr.at[batch_of(pos)])
        weigh(xp, wed_p, 8, pos)
        at = window(pos, core)[1]

        def classes(dy, carry):
            for j in range(2):
                class_sum(pos, at, dy, j)
            return carry

        lax.fori_loop(0, 4, classes, 0, unroll=True)
        done.add(ORDER[pos])
        for i, (t, make, place, rb, ra, needs) in enumerate(sends):
            if i not in sent and done.issuperset(needs):
                sent.add(i)
                encode(QS[t].at[place], S[t][ra, rb], *counts_of(t, ra))
                if make is own1 and pos < HOLD:
                    held.append((t, rb))
                else:
                    make(t, rb).start()
        if pos == HOLD:
            for t, rb in held:
                own1(t, rb).start()

    for t, rb in ((0, 2), (1, 2), (0, 1), (1, 1), (0, 3), (2, 2), (1, 3), (0, 0), (1, 0), (2, 1)):
        far1(t, rb).wait_recv()
        ra = 1 if rb >= 2 else 3
        v, c = decode(Q1[t].at[rb], 4 * STREAM_ROWS[t])
        encode(QS[t].at[8 + rb], S[t][ra, rb] + v, *[n + c for n in counts_of(t, ra)])
        comb1(t, rb).start()
    kept = [None] * 3
    waited = set()

    def wait_ring(t, rb):
        if (t, rb) not in waited:
            waited.add((t, rb))
            wait_bytes(QD[t].at[rb, pl.ds(0, arrivals(t, rb))], sem_rd.at[t, rb])

    wait_ring(0, 2)
    wait_ring(1, 2)
    counts = None
    for t, rb in ((0, 2), (1, 2), (2, 3), (0, 1), (1, 1), (2, 2), (2, 1), (0, 3), (1, 3), (0, 0), (2, 0), (1, 0)):
        wait_ring(t, rb)
        r = STREAM_ROWS[t]
        total = S[t][0, rb]
        seen = chip_counts(0) if t == 2 else None
        for side in range(arrivals(t, rb)):
            v, c = decode(QD[t].at[rb, side], 4 * r)
            total = total + v
            if t == 2:
                seen = seen + c
        if t == 2 and counts is None:
            counts = seen
        more = (counts,) if t == 2 else ()
        for rc in (2, 1, 3, 0):
            part = total[rc * r:(rc + 1) * r]
            if rb or rc:
                encode(QT[t].at[rb * 4 + rc - 1], part, *more)
                plane(t, rb, rc).start()
            else:
                kept[t] = part
    final = []
    for t in (0, 1, 2):
        wait_bytes(QF[t], sem_rf.at[t])
        total = kept[t]
        for m in range(15):
            v, c = decode(QF[t].at[m], STREAM_ROWS[t])
            total = total + v
            if t == 2:
                counts = counts + c
        final.append(total)
    tail, heads = final[2], final[:2]

    counts_lane = lax.broadcasted_iota(jnp.int32, (1, 128), 1)
    even = lax.rem(lax.broadcasted_iota(jnp.int32, (ROWS, 128), 0), 2) == 0
    own_at = window(PIECES - 1, core)[1]
    totals = []
    for j in range(2):
        row = counts[j:j + 1]
        total = jnp.zeros((ROWS, 128), F32)
        for w in range(WEDGES):
            n = jnp.sum(jnp.where(counts_lane == w, row, 0.0), axis=1, keepdims=True)
            a = wexp[PIECES - 1, w, pl.ds(own_at, ROWS), :]
            total = total + n * (a * a)
        totals.append(total)
        summed = jnp.concatenate([heads[j], tail[j * TAIL:(j + 1) * TAIL]], axis=0)
        avg = summed / (total + 1.0)
        avg_ref[j] = avg[0:2 * NB].reshape(NB, 2, 128)
    tot_ref[...] = jnp.where(even, totals[0], totals[1])[0:2 * NB].reshape(NB, 2, 128)
    for t in range(3):
        wait_bytes(QS[t], sem_s1.at[t])
        wait_bytes(QT[t], sem_s2.at[t])
    wait_bytes(xp, sem_ps)
    lab_copy.wait_send()
    wed_copy.wait_send()


def put_out(avg_ref, tot_ref, avg_out, tot_out, sems):
    one = pltpu.make_async_copy(avg_ref, avg_out, sems.at[0])
    two = pltpu.make_async_copy(tot_ref, tot_out, sems.at[1])
    one.start()
    two.start()
    one.wait()
    two.wait()


def per_device(particles, labels, wedge_index, wedge_table):
    x = particles.reshape(PDEV, 2, 32 * NB, 128).transpose(0, 2, 1, 3)
    x = x.reshape(PDEV, 64 * NB, 128)
    lab = labels.reshape(PDEV)
    hbm = pl.BlockSpec(memory_space=pltpu.HBM)
    vmem = pl.BlockSpec(memory_space=pltpu.VMEM)
    dma = pltpu.SemaphoreType.DMA
    V = pltpu.VMEM

    def per_stream(*lead):
        return [V((*lead, 4 * r, 128), F32) for r in STREAM_ROWS]

    def coded(*lead):
        return [V((*lead, 4 * r + extra, 128), jnp.int16)
                for r, extra in zip(STREAM_ROWS, (8, 8, 16))]

    shapes = (jax.ShapeDtypeStruct((2, NB, 2, 128), F32),
              jax.ShapeDtypeStruct((NB, 2, 128), F32))
    avg, tot = pl.pallas_call(
        kernel,
        out_shape=shapes,
        in_specs=[hbm] * 4,
        out_specs=(vmem, vmem),
        scratch_shapes=[
            V((PIECES, PDEV, WINDOW, 128), BF16),
            V((PIECES, PDEV, WINDOW, 128), BF16),
            V((PIECES * 16 + 1, WROWS, 128), F32),
            V((PIECES, WEDGES, NB * 128), F32),
            V((PIECES, WEDGES, WROWS, 128), F32),
            *[pltpu.SMEM((PDEV,), jnp.int32)] * 4,
            pltpu.SMEM((32,), jnp.int32),
            pltpu.SMEM((32,), jnp.int32),
            *per_stream(4, 4),
            *coded(12), *coded(4), *coded(4, 3),
            *[V((15, HEAD + 8, 128), jnp.int16)] * 6,
            dma((4,)), dma((4,)), dma((2,)), dma(()), dma((9,)), dma((2,)), dma((2,)),
            dma((3,)), dma((3,)), dma((3, 4)), dma((3, 4)), dma((3,)),
        ],
        compiler_params=pltpu.CompilerParams(
            collective_id=0, has_side_effects=True, vmem_limit_bytes=44 * 1024 * 1024),
        name="class_sums",
    )(*[pltpu.with_memory_space_constraint(a, pltpu.HBM) for a in (lab, wedge_index, x, wedge_table)])
    avg, tot = pl.pallas_call(
        put_out,
        out_shape=shapes,
        in_specs=[vmem] * 2,
        out_specs=(hbm, hbm),
        scratch_shapes=[dma((2,))],
        compiler_params=pltpu.CompilerParams(vmem_limit_bytes=1024 * 1024),
        name="put_out",
    )(avg, tot)
    avg = avg.transpose(0, 2, 1, 3).reshape(2, 2, NB * 128)
    tot = tot.transpose(1, 0, 2).reshape(2, NB * 128)
    return avg, tot


def solution(mesh):
    return jax.shard_map(
        per_device,
        mesh=mesh,
        in_specs=(P(("cls", "dom"), None, None), P(("cls", "dom"), None), P(("cls", "dom")), P()),
        out_specs=(P("cls", None, "dom"), P("cls", "dom")),
        check_vma=False,
    )
```
